32 devices in a mesh: data: 1 (over z), col: 4 (over y), row: 8 (over x, core).
Axes of the slice: x: 4, y: 4, z: 1, core: 2. Of those that a mesh axis runs over, the one named last changes fastest.
The devices are a block of a 4x4x8 slice.
Arguments:
- residual: bfloat16 [4096, 4096], P('data', 'row')
- gain_mlp: float32 [4096], P('row')
- gain_attn: float32 [4096], P('row')
- w_gate: bfloat16 [4096, 16384], P(None, ('col', 'row'))
- w_up: bfloat16 [4096, 16384], P(None, ('col', 'row'))
- w_down: bfloat16 [16384, 4096], P('col', 'row')
- w_qkv: bfloat16 [4096, 4608], P(None, ('col', 'row'))
Outputs:
- output 1: bfloat16 [4096, 4096], P('data', 'row')
- output 2: bfloat16 [4096, 4608], P('data', ('col', 'row'))
All inputs are finite; a program needn't handle non-finite values.
Results may differ from the reference program's by a relative error of at most 0.00402297.
Values are sent between devices in bfloat16 or wider.
A program may use at most 768 MiB of HBM per device.

```python
import math
import jax
import jax.numpy as jnp
from jax import lax

TOKENS = 4096
D = 4096
FF = 16384
HEADS = 16
KV_HEADS = 1
HEAD_DIM = 256
QKV_WIDTH = (HEADS + 2 * KV_HEADS) * HEAD_DIM
NORM_EPS = 1e-6


def setup_inputs(seed: int = 0, part: int = 0) -> dict:
    key_list = jax.random.split(jax.random.key(seed), 8)
    tok_keys = jax.random.split(jax.random.fold_in(key_list[0], part), 3)
    base_vals = jax.random.normal(tok_keys[0], (TOKENS, D), jnp.float32)
    tok_scale = jnp.exp(jax.random.uniform(tok_keys[1], (TOKENS, 1), jnp.float32, -1.0, 1.0))
    wave_amps = jax.random.normal(tok_keys[2], (TOKENS, 2), jnp.float32)
    angles = jnp.arange(D, dtype=jnp.float32) * (2.0 * math.pi / D)
    profile = jnp.exp(0.7 * (wave_amps[:, 0:1] * jnp.cos(angles) + wave_amps[:, 1:2] * jnp.sin(angles)))
    residual = (base_vals * tok_scale * profile).astype(jnp.bfloat16)
    gain_mlp = jax.random.uniform(key_list[1], (D,), jnp.float32, 0.4, 1.6)
    gain_attn = jax.random.uniform(key_list[2], (D,), jnp.float32, 0.4, 1.6)
    w_gate = (jax.random.normal(key_list[3], (D, FF), jnp.float32) * D ** -0.5).astype(jnp.bfloat16)
    w_up = (jax.random.normal(key_list[4], (D, FF), jnp.float32) * D ** -0.5).astype(jnp.bfloat16)
    w_down = (jax.random.normal(key_list[5], (FF, D), jnp.float32) * FF ** -0.5).astype(jnp.bfloat16)
    w_qkv = (jax.random.normal(key_list[6], (D, QKV_WIDTH), jnp.float32) * D ** -0.5).astype(jnp.bfloat16)
    return {'residual': residual, 'gain_mlp': gain_mlp, 'gain_attn': gain_attn, 'w_gate': w_gate, 'w_up': w_up, 'w_down': w_down, 'w_qkv': w_qkv}


def rms_normed(rows, gain):
    rows_f = rows.astype(jnp.float32)
    row_scale = lax.rsqrt(jnp.mean(rows_f * rows_f, axis=1, keepdims=True) + NORM_EPS)
    return (rows_f * row_scale * gain).astype(jnp.bfloat16)


def reference(residual, gain_mlp, gain_attn, w_gate, w_up, w_down, w_qkv):
    normed = rms_normed(residual, gain_mlp)
    gate_val = jnp.dot(normed, w_gate, preferred_element_type=jnp.float32)
    up_val = jnp.dot(normed, w_up, preferred_element_type=jnp.float32)
    act_val = (jax.nn.silu(gate_val) * up_val).astype(jnp.bfloat16)
    down_val = jnp.dot(act_val, w_down, preferred_element_type=jnp.float32)
    resid_next = (residual.astype(jnp.float32) + down_val).astype(jnp.bfloat16)
    normed_next = rms_normed(resid_next, gain_attn)
    qkv_out = jnp.dot(normed_next, w_qkv, preferred_element_type=jnp.float32).astype(jnp.bfloat16)
    return (resid_next, qkv_out)
```

```python
import functools

import jax
import jax.numpy as jnp
from jax import lax
from jax.experimental import pallas as pl
from jax.experimental.pallas import tpu as pltpu
from jax.sharding import PartitionSpec as P

NORM_EPS = 1e-6
MESH = pl.DeviceIdType.MESH
BF16 = jnp.bfloat16
F32 = jnp.float32
ANY = pl.BlockSpec(memory_space=pl.ANY)
VMEM = pl.BlockSpec(memory_space=pltpu.VMEM)
DMA = pltpu.SemaphoreType.DMA
LIMIT = 64 * 1024 * 1024 - 128 * 1024

NX, NY = 4, 4
SY = 5
SX = 12
SY_CHUNKS = ((0, 1), (1, 2), (3, 2))
SX_CHUNKS = tuple((i, 2) for i in range(0, SX, 2))
PIECES = NY * SY + SX


def place():
    row, y = lax.axis_index("row"), lax.axis_index("col")
    return lax.div(row, 2), lax.rem(row, 2), row, y


def around(i, n):
    return lax.rem(i + 1, n), lax.rem(i + n - 1, n), lax.rem(i + 2, n)


def greet(peers):
    barrier = pltpu.get_barrier_semaphore()
    for row, y in peers:
        pl.semaphore_signal(barrier, inc=1, device_id={"row": row, "col": y}, device_id_type=MESH)
    pl.semaphore_wait(barrier, len(peers))


def to(src, dst, send, recv, row, y):
    return pltpu.make_async_remote_copy(src, dst, send, recv, device_id={"row": row, "col": y}, device_id_type=MESH)


def norm_rows(load, gains, which, store, n_ent, width):
    acc = None
    for e in range(n_ent):
        v = load(e).astype(F32)
        acc = v * v if acc is None else acc + v * v
    scale = lax.rsqrt(jnp.sum(acc, axis=1, keepdims=True) / (n_ent * width) + NORM_EPS)
    for e in range(n_ent):
        store(e, (load(e).astype(F32) * scale * gains[e, which : which + 1, :]).astype(BF16))


def k1_names():
    names = []
    for k in range(len(SY_CHUNKS)):
        names += [f"{n}_{k}" for n in ("xp", "xm", "xpf", "xmf", "yp1", "yp2", "yp3", "ym1", "ym2", "ym3")]
        names += [f"{n}_{k}" for n in ("ypf1", "ypf3", "ymf2", "ymf3")]
    for k in range(len(SX_CHUNKS)):
        names += [f"{n}_{k}" for n in ("sp", "sm", "spf", "smf")]
    names += [f"d_{s}" for s in range(NY + 1)]
    names += [f"g_{d}" for d in range(1, 2 * NX)]
    names += ["wg", "wu"]
    return names


K1_TILES = (
    (("s", 0), ("s", 1)),
    (("s", 2), ("m", 0)),
    (("p", 0), ("s", 3)),
    (("s", 4), ("m", 1)),
    (("m", 2), ("p", 1)),
    (("p", 2), ("x", 0)),
    (("x", 1), ("o", 0)),
    (("x", 2), ("x", 3)),
    (("x", 4), ("x", 5)),
    (("m", 3), ("m", 4)),
    (("p", 3), ("p", 4)),
    (("o", 1), ("o", 2)),
    (("x", 6), ("x", 7)),
    (("x", 8), ("x", 9)),
    (("o", 3), ("o", 4)),
    (("x", 10), ("x", 11)),
)


def k1_plan():
    both = lambda n, k: [f"{n}p_{k}", f"{n}m_{k}"]
    bothf = lambda n, k: [f"{n}pf_{k}", f"{n}mf_{k}"]
    ypair = lambda k: [f"{n}_{k}" for n in ("yp1", "yp2", "ym1", "ym2")]
    ytrip = lambda k: [f"{n}_{k}" for n in ("yp3", "ym3")]
    yfwd = lambda k: [f"{n}_{k}" for n in ("ypf1", "ypf3", "ymf2", "ymf3")]
    w, s = "w", "s"
    return {
        -1: [
            (s, both("x", 0) + both("x", 1)),
            (w, both("x", 0)),
            (s, bothf("x", 0) + ypair(0) + both("x", 2)),
            (w, bothf("x", 0)),
            (s, ytrip(0)),
            (w, both("x", 1)),
            (s, bothf("x", 1) + ypair(1)),
            ("rest", []),
            (s, both("s", 0)),
            (w, both("x", 2)),
            (s, bothf("x", 2) + both("s", 1)),
            (w, bothf("x", 1)),
            (s, ytrip(1)),
        ],
        1: [(w, ypair(0) + ytrip(0)), (s, yfwd(0))],
        2: [
            (w, bothf("x", 2)),
            (s, ypair(2) + ytrip(2)),
            (w, both("s", 0)),
            (s, bothf("s", 0) + both("s", 2)),
        ],
        3: [(w, ypair(1) + ytrip(1)), (s, yfwd(1))],
        4: [(w, both("s", 1)), (s, bothf("s", 1) + both("s", 3))],
        5: [(w, bothf("s", 0))],
        6: [(w, yfwd(0))],
        7: [(w, bothf("s", 1) + both("s", 2)), (s, bothf("s", 2) + both("s", 4))],
        8: [(w, bothf("s", 2) + both("s", 3)), (s, bothf("s", 3) + both("s", 5))],
        9: [(w, ypair(2) + ytrip(2)), (s, yfwd(2))],
        10: [(w, both("s", 4)), (s, bothf("s", 4))],
        11: [(w, yfwd(1))],
        12: [(w, bothf("s", 3) + both("s", 5)), (s, bothf("s", 5))],
        13: [(w, bothf("s", 4))],
        14: [(w, yfwd(2))],
        15: [(w, bothf("s", 5))],
    }


def k1(x_ref, g_ref, wg_ref, wu_ref, a_ref, xres_ref, gout_ref, xb, wgb, wub, nt, gb, send, recv, loc):
    x, c, row, y = place()
    xp, xm, x2 = around(x, NX)
    yp, ym, y2 = around(y, NY)
    n_ent = 2 * NX
    half, width, ff = xb.shape[1], xb.shape[2], wgb.shape[2]
    piece = half // PIECES
    ids = {n: i for i, n in enumerate(k1_names())}
    partner = 2 * x + 1 - c

    copies = {}

    def define(name, src, dst, to_row, to_y):
        i = ids[name]
        copies[name] = to(src, dst, send.at[i], recv.at[i], to_row, to_y)

    def ring(name, ents, rows, to_row, to_y):
        ref = xb.at[ents, rows]
        define(name, ref, ref, to_row, to_y)

    blk = lambda i: pl.ds(2 * i, 2)
    ent = lambda i: pl.ds(i, 1)
    row_p, row_m = 2 * xp + c, 2 * xm + c
    for k, (o, n) in enumerate(SY_CHUNKS):
        rows = lambda j: pl.ds(pl.multiple_of((j * SY + o) * piece, piece), n * piece)
        ring(f"xp_{k}", blk(x), rows(y), row_p, y)
        ring(f"xm_{k}", blk(x), rows(y), row_m, y)
        ring(f"xpf_{k}", ent(2 * xm), rows(y), row_p, y)
        ring(f"xmf_{k}", ent(2 * xp + 1), rows(y), row_m, y)
        for tag, j in (("yp", yp), ("ym", ym)):
            for i, b in enumerate((xm, xp, x2)):
                ring(f"{tag}{i + 1}_{k}", blk(b), rows(y), row, j)
        ring(f"ypf1_{k}", blk(xm), rows(ym), row, yp)
        ring(f"ypf3_{k}", ent(2 * x2), rows(ym), row, yp)
        ring(f"ymf2_{k}", blk(xp), rows(yp), row, ym)
        ring(f"ymf3_{k}", ent(2 * x2 + 1), rows(yp), row, ym)
    for k, (o, n) in enumerate(SX_CHUNKS):
        rows = pl.ds((NY * SY + o) * piece, n * piece)
        ring(f"sp_{k}", blk(x), rows, row_p, y)
        ring(f"sm_{k}", blk(x), rows, row_m, y)
        ring(f"spf_{k}", ent(2 * xm), rows, row_p, y)
        ring(f"smf_{k}", ent(2 * xp + 1), rows, row_m, y)

    regions = [(y * SY * piece, SY * piece), (NY * SY * piece, SX * piece)]
    regions += [(lax.rem(y + d, NY) * SY * piece, SY * piece) for d in range(1, NY)]
    local = []
    for s, (start, n) in enumerate(regions):
        start = pl.multiple_of(start, piece) if s != 1 else start
        there = xb.at[row, pl.ds(start, n)]
        local.append(pltpu.make_async_copy(x_ref.at[pl.ds(c * half + start, n)], there, loc.at[s]))
        define(f"d_{s}", x_ref.at[pl.ds((1 - c) * half + start, n)], there, partner, y)
    for d in range(1, n_ent):
        define(f"g_{d}", g_ref, gb.at[row], lax.rem(row + d, n_ent), y)
    define("wg", wg_ref, wgb.at[c], partner, y)
    define("wu", wu_ref, wub.at[c], partner, y)
    local.append(pltpu.make_async_copy(g_ref, gb.at[row], loc.at[NY + 1]))
    local.append(pltpu.make_async_copy(wg_ref, wgb.at[c], loc.at[NY + 2]))
    local.append(pltpu.make_async_copy(wu_ref, wub.at[c], loc.at[NY + 3]))
    for cp in local:
        cp.start()

    greet([(lax.rem(row + d, n_ent), y) for d in range(1, n_ent)] + [(row, yp), (row, ym)])

    for n in [f"d_{s}" for s in range(NY + 1)] + [f"g_{d}" for d in range(1, n_ent)] + ["wg", "wu"]:
        copies[n].start()

    def act(steps):
        for what, names in steps:
            if what == "rest":
                for s in range(1, NY + 1):
                    local[s].wait()
                    copies[f"d_{s}"].wait_recv()
            for n in names:
                if what == "s":
                    copies[n].start()
                elif what == "w":
                    copies[n].wait_recv()

    plan = k1_plan()
    local[0].wait()
    copies["d_0"].wait_recv()
    act(plan[-1])
    for cp in local[NY + 1 :]:
        cp.wait()
    for n in [f"g_{d}" for d in range(1, n_ent)] + ["wg", "wu"]:
        copies[n].wait_recv()

    base = {"s": y * SY, "m": ym * SY, "p": yp * SY, "o": y2 * SY, "x": NY * SY}
    per_tile = len(K1_TILES[0])

    def tile(s, _):
        for k in sorted(plan):
            if k >= 0:
                pl.when(s == k)(functools.partial(act, plan[k]))
        starts = []
        for i in range(per_tile):
            at = base[K1_TILES[0][i][0]] + K1_TILES[0][i][1]
            for k in range(1, len(K1_TILES)):
                kind, j = K1_TILES[k][i]
                at = jnp.where(s == k, base[kind] + j, at)
            starts.append(at * piece)

        for i, at in enumerate(starts):

            def sixteen(g, _, at=at, i=i):
                r = pl.multiple_of(at + g * 16, 16)
                d = pl.multiple_of(i * piece + g * 16, 16)

                def store(e, v):
                    nt[pl.ds(d, 16), e * width : (e + 1) * width] = v

                norm_rows(lambda e: xb[e, pl.ds(r, 16), :], gb, 0, store, n_ent, width)
                return 0

            lax.fori_loop(0, piece // 16, sixteen, 0)

        step = min(256, ff)
        for h in range(2):
            for col in range(0, ff, step):
                gate = jnp.dot(nt[...], wgb[h, :, col : col + step], preferred_element_type=F32)
                up = jnp.dot(nt[...], wub[h, :, col : col + step], preferred_element_type=F32)
                act_val = (gate * lax.logistic(gate) * up).astype(BF16)
                for i, at in enumerate(starts):
                    r = pl.multiple_of(at, 16)
                    a_ref[pl.ds(r, piece), h * ff + col : h * ff + col + step] = act_val[i * piece : (i + 1) * piece]
        return 0

    lax.fori_loop(0, len(K1_TILES), tile, 0)

    def keep(j, _):
        r = pl.multiple_of(j * NY * piece + y * piece, 16)
        for h in range(2):
            xres_ref[h, j] = xb[2 * x + h, pl.ds(r, piece), :]
        return 0

    lax.fori_loop(0, PIECES // NY, keep, 0)
    gout_ref[...] = gb[...]
    for n in ids:
        copies[n].wait_send()


AP, AM, APF, AMF, S1L, S1R, FL, FR, GL, GR = range(10)
QP, QM, QPF, QMF, QD0, QD1, QD2, QD3A, QD3B, WD = range(10)
RP, RM = 0, 2
RPF, RMF, RD = 4, 5, 6


def k2(
    a_ref, wd_ref, xres_ref, wq_ref, resid_ref, xn_ref, wqa_ref,
    aall, wdb, pbuf, r1, rf, send, recv, qsend, qrecv, rsend, rrecv, loc, rloc,
):
    x, c, row, y = place()
    xp, xm, _ = around(x, NX)
    yp, ym, y2 = around(y, NY)
    n_tiles = PIECES // NY
    piece, width = pbuf.shape[3], pbuf.shape[4]
    rows_n = NY * piece
    ffc = a_ref.shape[1]
    row_p, row_m, partner = 2 * xp + c, 2 * xm + c, 2 * x + 1 - c

    def cols(i):
        return pl.ds(pl.multiple_of(i * ffc, 128), ffc)

    first = pltpu.make_async_copy(a_ref.at[pl.ds(0, 2 * rows_n)], aall.at[pl.ds(0, 2 * rows_n), cols(x)], loc.at[0])
    rest_n = a_ref.shape[0] - 2 * rows_n
    rest = pltpu.make_async_copy(
        a_ref.at[pl.ds(2 * rows_n, rest_n)], aall.at[pl.ds(2 * rows_n, rest_n), cols(x)], loc.at[1]
    )
    wd_own = pltpu.make_async_copy(wd_ref, wdb.at[c], loc.at[2])
    first.start()
    wd_own.start()
    rest.start()

    greet([(row_p, y), (row_m, y), (partner, y), (row, yp), (row, ym), (partner, yp), (partner, ym)])

    def ring(kind, j, src, dst, to_row, to_y):
        return to(src, dst, send.at[kind, j], recv.at[kind, j], to_row, to_y)

    def own(j):
        ref = aall.at[pl.ds(pl.multiple_of(j * rows_n, 16), rows_n), cols(x)]
        return ring(AP, j, ref, ref, row_p, y), ring(AM, j, ref, ref, row_m, y)

    def onward(j):
        h = rows_n // 2
        up = aall.at[pl.ds(pl.multiple_of(j * rows_n, 16), h), cols(xm)]
        down = aall.at[pl.ds(pl.multiple_of(j * rows_n + h, 16), h), cols(xp)]
        return ring(APF, j, up, up, row_p, y), ring(AMF, j, down, down, row_m, y)

    def early(j):
        return (
            ring(S1L, j, pbuf.at[j, 0, y2], r1.at[j, 0], row, yp),
            ring(S1R, j, pbuf.at[j, 1, y2], r1.at[j, 1], row, ym),
            ring(FR, j, pbuf.at[j, 1, yp], rf.at[j, 1], row, yp),
            ring(GL, j, pbuf.at[j, 0, ym], rf.at[j, 2], row, ym),
        )

    def late(j):
        return (
            ring(FL, j, pbuf.at[j, 0, yp], rf.at[j, 0], row, yp),
            ring(GR, j, pbuf.at[j, 1, ym], rf.at[j, 3], row, ym),
        )

    def q(i, src, dst, to_row, to_y):
        return to(src, dst, qsend.at[i], qrecv.at[i], to_row, to_y)

    qn = wq_ref.shape[0]
    cut = (qn // 2 + 15) // 16 * 16
    lo, hi = pl.ds(0, cut), pl.ds(cut, qn - cut)
    mine, b_m, b_p, b_2 = 2 * y + c, 2 * ym + c, 2 * yp + c, 2 * y2 + c
    qs = {
        QP: q(QP, wq_ref, wqa_ref.at[mine], row, yp),
        QM: q(QM, wq_ref, wqa_ref.at[mine], row, ym),
        QPF: q(QPF, wqa_ref.at[b_m, lo], wqa_ref.at[b_m, lo], row, yp),
        QMF: q(QMF, wqa_ref.at[b_p, hi], wqa_ref.at[b_p, hi], row, ym),
        QD0: q(QD0, wq_ref, wqa_ref.at[mine], partner, y),
        QD1: q(QD1, wqa_ref.at[b_m], wqa_ref.at[b_m], partner, y),
        QD2: q(QD2, wqa_ref.at[b_p], wqa_ref.at[b_p], partner, y),
        QD3A: q(QD3A, wqa_ref.at[b_2, lo], wqa_ref.at[b_2, lo], partner, y),
        QD3B: q(QD3B, wqa_ref.at[b_2, hi], wqa_ref.at[b_2, hi], partner, y),
        WD: q(WD, wd_ref, wdb.at[c], partner, y),
    }

    def out(jj):
        two = pl.ds(2 * jj, 2)
        there = resid_ref.at[c, two, y]
        sends = []
        for h in range(2):
            src = xn_ref.at[h, two]
            sends.append(to(src, there, rsend.at[RP + h, jj], rrecv.at[RP + c, jj], 2 * x + h, yp))
            sends.append(to(src, there, rsend.at[RM + h, jj], rrecv.at[RM + c, jj], 2 * x + h, ym))
        sends.append(to(xn_ref.at[1 - c, two], there, rsend.at[RD, jj], rrecv.at[RD, jj], partner, y))
        return sends

    def out_own(jj):
        two = pl.ds(2 * jj, 2)
        return pltpu.make_async_copy(xn_ref.at[c, two], resid_ref.at[c, two, y], rloc.at[jj])

    def arrived(jj):
        two = pl.ds(2 * jj, 2)
        return [
            to(xn_ref.at[0, two], resid_ref.at[0, two, y], rsend.at[i, jj], rrecv.at[i, jj], row, yp) for i in range(4)
        ]

    def relay(jj):
        two = pl.ds(2 * jj, 2)
        up, down = resid_ref.at[0, two, ym], resid_ref.at[1, two, yp]
        return (
            to(up, up, rsend.at[RPF, jj], rrecv.at[RPF, jj], row, yp),
            to(down, down, rsend.at[RMF, jj], rrecv.at[RMF, jj], row, ym),
        )

    def start(cps):
        for cp in cps:
            cp.start()

    def got(cps):
        for cp in cps:
            cp.wait_recv()

    def step2(j):
        got(early(j)[:2])
        for r in range(0, piece, 16):
            s = pl.ds(r, 16)
            pbuf[j, 0, yp, s, :] = pbuf[j, 0, yp, s, :] + r1[j, 0, s, :]
            pbuf[j, 1, ym, s, :] = pbuf[j, 1, ym, s, :] + r1[j, 1, s, :]
        start(late(j))

    def final(j):
        got(early(j)[2:] + late(j))
        for h in range(2):
            for r in range(0, piece, 16):
                s = pl.ds(r, 16)
                total = pbuf[j, h, y, s, :] + rf[j, h, s, :] + rf[j, 2 + h, s, :]
                xn_ref[h, j, s, :] = (xres_ref[h, j, s, :].astype(F32) + total).astype(BF16)

    def relay_now(jj):
        got(arrived(jj))
        start(relay(jj))

    first.wait()
    start(own(0))
    qs[WD].start()
    start(own(1))
    start([qs[QP], qs[QM], qs[QD0]])
    rest.wait()
    wd_own.wait()
    qs[WD].wait_recv()

    step = min(256, width)

    def tile(j, _):
        @pl.when(j < n_tiles)
        def _():
            got(own(j))
            start(onward(j))

        @pl.when(j + 2 < n_tiles)
        def _():
            start(own(j + 2))

        @pl.when(j == 2)
        def _():
            got([qs[QP], qs[QM]])
            start([qs[QPF], qs[QMF], qs[QD1], qs[QD2]])

        @pl.when(j == 5)
        def _():
            got([qs[QPF], qs[QMF]])
            start([qs[QD3A], qs[QD3B]])

        @pl.when((j >= 1) & (j <= n_tiles))
        def _():
            step2(j - 1)

        @pl.when(j >= 2)
        def _():
            final(j - 2)

        @pl.when((j >= 3) & (lax.rem(j, 2) == 1))
        def _():
            jj = lax.div(j - 3, 2)
            start(out(jj))
            out_own(jj).start()

        @pl.when((j >= 5) & (lax.rem(j, 2) == 1))
        def _():
            relay_now(lax.div(j - 5, 2))

        @pl.when(j < n_tiles)
        def _():
            got(onward(j))
            lhs = pl.ds(pl.multiple_of(j * rows_n, 16), rows_n)
            for h in range(2):
                for col in range(0, width, step):
                    part = jnp.dot(aall[lhs, :], wdb[h, :, col : col + step], preferred_element_type=F32)
                    for i in range(NY):
                        pbuf[j, h, i, :, col : col + step] = part[i * piece : (i + 1) * piece]
            start(early(j))

        return 0

    lax.fori_loop(0, n_tiles + 2, tile, 0)
    relay_now(n_tiles // 2 - 1)

    got([qs[i] for i in (QD0, QD1, QD2, QD3A, QD3B)])

    def settle(j, _):
        for cp in own(j) + onward(j) + early(j) + late(j):
            cp.wait_send()
        return 0

    lax.fori_loop(0, n_tiles, settle, 0)

    def settle_out(jj, _):
        for cp in out(jj) + list(relay(jj)):
            cp.wait_send()
        got([out(jj)[-1]] + list(relay(jj)))
        out_own(jj).wait()
        return 0

    lax.fori_loop(0, n_tiles // 2, settle_out, 0)
    for i in qs:
        qs[i].wait_send()


def k3(xn_ref, gb_ref, wq_ref, wqa_ref, out_ref, xg, wqb, nt, ob, send, recv, osend, orecv, loc, oloc):
    x, c, row, y = place()
    xp, xm, _ = around(x, NX)
    n_ent = 2 * NX
    n_chunks = xg.shape[1] // 2
    piece, width = xg.shape[2], xg.shape[3]
    row_p, row_m, partner = 2 * xp + c, 2 * xm + c, 2 * x + 1 - c
    mine = 2 * y + c

    own = pltpu.make_async_copy(xn_ref, xg.at[pl.ds(2 * x, 2)], loc.at[0])
    own.start()
    loads = [pltpu.make_async_copy(wq_ref, wqb.at[mine], loc.at[1])]
    for d in range(1, 2 * NY):
        b = lax.rem(mine + d, 2 * NY)
        loads.append(pltpu.make_async_copy(wqa_ref.at[b], wqb.at[b], loc.at[1 + d]))
    for cp in loads:
        cp.start()

    column = [(2 * x + h, lax.rem(y + d, NY)) for d in range(1, NY) for h in range(2)]
    greet([(row_p, y), (row_m, y), (partner, y)] + column)

    def ring(kind, q, ents, to_row):
        ref = xg.at[ents, pl.ds(2 * q, 2)]
        return to(ref, ref, send.at[kind, q], recv.at[kind, q], to_row, y)

    def mains(q):
        return ring(0, q, pl.ds(2 * x, 2), row_p), ring(1, q, pl.ds(2 * x, 2), row_m)

    def onward(q):
        return ring(2, q, pl.ds(2 * xm, 1), row_p), ring(3, q, pl.ds(2 * xp + 1, 1), row_m)

    def result(q, d, f):
        h = c if f == 0 else 1 - c
        i = 2 * d + f
        src, dst = ob.at[q, i], out_ref.at[c, pl.ds(2 * q, 2), y]
        if i == 0:
            return pltpu.make_async_copy(src, dst, oloc.at[q])
        return to(src, dst, osend.at[q, i], orecv.at[q, i], 2 * x + h, lax.rem(y + d, NY))

    own.wait()
    for q in range(n_chunks):
        for cp in mains(q):
            cp.start()
        if q == 0:
            for cp in mains(q):
                cp.wait_recv()
            for cp in onward(q):
                cp.start()
    for cp in loads:
        cp.wait()

    def chunk(q, _):
        for cp in onward(q):
            cp.wait_recv()

        @pl.when(q + 1 < n_chunks)
        def _():
            for cp in mains(q + 1):
                cp.wait_recv()
            for cp in onward(q + 1):
                cp.start()

        for t in range(2):

            def sixteen(g, _, t=t):
                r = pl.multiple_of(g * 16, 16)
                d = pl.multiple_of(t * piece + g * 16, 16)

                def store(e, v):
                    nt[pl.ds(d, 16), e * width : (e + 1) * width] = v

                norm_rows(lambda e: xg[e, 2 * q + t, pl.ds(r, 16), :], gb_ref, 1, store, n_ent, width)
                return 0

            lax.fori_loop(0, piece // 16, sixteen, 0)

        for d in (2, 1, 3, 0):
            for f in range(2):
                h = c if f == 0 else 1 - c
                b = 2 * lax.rem(y + d, NY) + h
                part = lax.dot_general(nt[...], wqb[b], (((1,), (1,)), ((), ())), preferred_element_type=F32)
                part = part.astype(BF16)
                for t in range(2):
                    ob[q, 2 * d + f, t] = part[t * piece : (t + 1) * piece]
                result(q, d, f).start()
        return 0

    lax.fori_loop(0, n_chunks, chunk, 0)

    def settle(q, _):
        for cp in mains(q) + onward(q):
            cp.wait_send()
        for d in range(NY):
            for f in range(2):
                result(q, d, f).wait()
        return 0

    lax.fori_loop(0, n_chunks, settle, 0)


def solution(mesh):
    assert mesh.shape["row"] == 2 * NX and mesh.shape["col"] == NY
    tok_spec, gain_spec = P("data", "row"), P("row")
    wide_spec, down_spec, qkv_spec = P(None, ("col", "row")), P("col", "row"), P("data", ("col", "row"))

    def params(i):
        return pltpu.CompilerParams(collective_id=i, has_side_effects=True, vmem_limit_bytes=LIMIT)

    def per_device(residual, gain_mlp, gain_attn, w_gate, w_up, w_down, w_qkv):
        tokens, width = residual.shape
        hidden, ff = w_gate.shape
        qn = w_qkv.shape[1]
        half = tokens // 2
        piece = half // PIECES
        tiles = PIECES // NY
        n_ent = 2 * NX
        gains = jnp.concatenate([gain_mlp[None], gain_attn[None], jnp.zeros((6, width), F32)])
        wq = w_qkv.T
        n1 = len(k1_names())
        act, xres, gb = pl.pallas_call(
            k1,
            name="gather_mlp_in",
            out_shape=[
                jax.ShapeDtypeStruct((half, 2 * ff), BF16),
                jax.ShapeDtypeStruct((2, tiles, piece, width), BF16),
                jax.ShapeDtypeStruct((n_ent, 8, width), F32),
            ],
            in_specs=[ANY] * 4,
            out_specs=[VMEM] * 3,
            scratch_shapes=[
                pltpu.VMEM((n_ent, half, width), BF16),
                pltpu.VMEM((2, hidden, ff), BF16),
                pltpu.VMEM((2, hidden, ff), BF16),
                pltpu.VMEM((len(K1_TILES[0]) * piece, hidden), BF16),
                pltpu.VMEM((n_ent, 8, width), F32),
                DMA((n1,)),
                DMA((n1,)),
                DMA((NY + 4,)),
            ],
            compiler_params=params(1),
        )(residual, gains, w_gate, w_up)
        resid, xn, wqa = pl.pallas_call(
            k2,
            name="gather_mlp_out",
            out_shape=[
                jax.ShapeDtypeStruct((2, tiles, NY, piece, width), BF16),
                jax.ShapeDtypeStruct((2, tiles, piece, width), BF16),
                jax.ShapeDtypeStruct((2 * NY, qn, hidden), BF16),
            ],
            in_specs=[ANY, ANY, VMEM, ANY],
            out_specs=[ANY, VMEM, ANY],
            scratch_shapes=[
                pltpu.VMEM((half, n_ent * ff), BF16),
                pltpu.VMEM((2, n_ent * ff, width), BF16),
                pltpu.VMEM((tiles, 2, NY, piece, width), F32),
                pltpu.VMEM((tiles, 2, piece, width), F32),
                pltpu.VMEM((tiles, 4, piece, width), F32),
                DMA((10, tiles)),
                DMA((10, tiles)),
                DMA((10,)),
                DMA((10,)),
                DMA((7, tiles // 2)),
                DMA((7, tiles // 2)),
                DMA((3,)),
                DMA((tiles // 2,)),
            ],
            compiler_params=params(2),
        )(act, w_down, xres, wq)
        (qkv,) = pl.pallas_call(
            k3,
            name="gather_qkv",
            out_shape=[jax.ShapeDtypeStruct((2, tiles, NY, piece, qn), BF16)],
            in_specs=[ANY, VMEM, ANY, ANY],
            out_specs=[ANY],
            scratch_shapes=[
                pltpu.VMEM((n_ent, tiles, piece, width), BF16),
                pltpu.VMEM((2 * NY, qn, hidden), BF16),
                pltpu.VMEM((2 * piece, hidden), BF16),
                pltpu.VMEM((tiles // 2, 2 * NY, 2, piece, qn), BF16),
                DMA((4, tiles // 2)),
                DMA((4, tiles // 2)),
                DMA((tiles // 2, 2 * NY)),
                DMA((tiles // 2, 2 * NY)),
                DMA((1 + 2 * NY,)),
                DMA((tiles // 2,)),
            ],
            compiler_params=params(3),
        )(xn, gb, wq, wqa)
        return resid.reshape(tokens, width), qkv.reshape(tokens, qn)

    return jax.shard_map(
        per_device,
        mesh=mesh,
        in_specs=(tok_spec, gain_spec, gain_spec, wide_spec, wide_spec, down_spec, wide_spec),
        out_specs=(tok_spec, qkv_spec),
        check_vma=False,
    )
```

```python
import functools

import jax
import jax.numpy as jnp
from jax import lax
from jax.experimental import pallas as pl
from jax.experimental.pallas import tpu as pltpu
from jax.sharding import PartitionSpec as P

NORM_EPS = 1e-6
MESH = pl.DeviceIdType.MESH
BF16 = jnp.bfloat16
F32 = jnp.float32
ANY = pl.BlockSpec(memory_space=pl.ANY)
VMEM = pl.BlockSpec(memory_space=pltpu.VMEM)
DMA = pltpu.SemaphoreType.DMA
LIMIT = 64 * 1024 * 1024 - 128 * 1024

NX, NY = 4, 4
PAIRS = 16
SY = 3
SX = PAIRS - NY * SY
EARLY = 2
TILES = PAIRS // 2
SHIFT = TILES - EARLY
CHUNKS = TILES // 2


def place():
    row, y = lax.axis_index("row"), lax.axis_index("col")
    return lax.div(row, 2), lax.rem(row, 2), row, y


def around(i, n):
    return lax.rem(i + 1, n), lax.rem(i + n - 1, n), lax.rem(i + 2, n)


def greet(peers):
    barrier = pltpu.get_barrier_semaphore()
    for row, y in peers:
        pl.semaphore_signal(barrier, inc=1, device_id={"row": row, "col": y}, device_id_type=MESH)
    pl.semaphore_wait(barrier, len(peers))


def to(src, dst, send, recv, row, y):
    return pltpu.make_async_remote_copy(src, dst, send, recv, device_id={"row": row, "col": y}, device_id_type=MESH)


def start(copies):
    for cp in copies:
        cp.start()


def got(copies):
    for cp in copies:
        cp.wait_recv()


def norm_rows(load, gains, which, store, n_ent, width):
    acc = None
    for e in range(n_ent):
        v = load(e).astype(F32)
        acc = v * v if acc is None else acc + v * v
    scale = lax.rsqrt(jnp.sum(acc, axis=1, keepdims=True) / (n_ent * width) + NORM_EPS)
    for e in range(n_ent):
        store(e, (load(e).astype(F32) * scale * gains[e, which : which + 1, :]).astype(BF16))


GROUPS = {
    "xp": ("xp", "xm"),
    "xf": ("xpf", "xmf"),
    "ya": ("yp1", "yp2", "ym1", "ym2"),
    "yb": ("yp3", "ym3"),
    "yf": ("ypf1", "ypf3", "ymf2", "ymf3"),
    "s": ("sp", "sm"),
    "sf": ("spf", "smf"),
    "a": ("ap", "am"),
    "af": ("apf", "amf"),
}
COUNTS = {"xp": SY, "xf": SY, "ya": SY, "yb": SY, "yf": SY, "s": SX, "sf": SX, "a": EARLY, "af": EARLY}

K1_TILES = ("s0", "m0", "s1", "s2", "p0", "x0", "o0", "x1", "m1", "x2", "x3", "p1", "m2", "p2", "o1", "o2")
K1_PLAN = (
    ("s", "xp0", "xp1", "xp2", "w", "xp0", "s", "xf0", "ya0", "s0", "w", "xp1", "s", "xf1", "w", "xp2", "s", "xf2", "w", "xf0", "s", "yb0", "ya1"),
    ("s", "s1", "w", "s0", "s", "sf0", "w", "ya0", "yb0", "s", "yf0"),
    ("w", "xf1", "s", "yb1", "ya2", "w", "xf2", "s", "yb2", "s2"),
    (),
    ("w", "s1", "s", "sf1"),
    ("s", "s3", "w", "sf0"),
    ("w", "s2", "s", "sf2", "w", "yf0"),
    ("w", "sf1"),
    ("w", "ya1", "yb1", "s", "yf1", "w", "s3", "s", "sf3", "a0"),
    ("w", "sf2"),
    ("w", "sf3"),
    ("s", "a1"),
    ("w", "ya2", "yb2", "s", "yf2"),
    ("w", "a0", "s", "af0"),
    ("w", "yf1"),
    ("w", "a1", "s", "af1", "w", "yf2"),
    ("w", "af0", "af1"),
)


def k1_steps(tokens):
    steps, what = [], None
    for token in tokens:
        if token in ("s", "w"):
            what = token
        else:
            steps.append((what, token))
    return steps


def k1_names():
    names = []
    for group, parts in GROUPS.items():
        for k in range(COUNTS[group]):
            for part in parts:
                names += [f"{part}{k}a", f"{part}{k}b"] if group == "xp" and k == 0 else [f"{part}{k}"]
    names += [f"d{s}" for s in range(NY + 1)]
    names += [f"g{d}" for d in range(1, 2 * NX)]
    return names + ["wg", "wu"]


def k1(x_ref, g_ref, wg_ref, wu_ref, a_ref, xres_ref, gout_ref, ag_ref, xb, wgb, wub, nt, gb, send, recv, loc):
    x, c, row, y = place()
    xp, xm, x2 = around(x, NX)
    yp, ym, y2 = around(y, NY)
    n_ent = 2 * NX
    piece, width, ff = xb.shape[3], xb.shape[4], wgb.shape[2]
    ids = {n: i for i, n in enumerate(k1_names())}
    partner = 2 * x + 1 - c
    row_p, row_m = 2 * xp + c, 2 * xm + c
    copies = {}

    def define(name, src, dst, to_row, to_y):
        i = ids[name]
        copies[name] = to(src, dst, send.at[i], recv.at[i], to_row, to_y)

    def ring(name, ents, where, to_row, to_y):
        ref = xb.at[(ents, *where)]
        define(name, ref, ref, to_row, to_y)

    blk = lambda i: pl.ds(2 * i, 2)
    ent = lambda i: pl.ds(i, 1)
    for k in range(SY):
        rows = lambda j: (pl.ds(j * SY + k, 1),)
        for part, j in (("xp", row_p), ("xm", row_m)):
            if k == 0:
                ring(f"{part}0a", ent(row), rows(y), j, y)
                ring(f"{part}0b", ent(partner), rows(y), j, y)
            else:
                ring(f"{part}{k}", blk(x), rows(y), j, y)
        ring(f"xpf{k}", ent(2 * xm), rows(y), row_p, y)
        ring(f"xmf{k}", ent(2 * xp + 1), rows(y), row_m, y)
        for tag, j in (("yp", yp), ("ym", ym)):
            for i, b in enumerate((xm, xp, x2)):
                ring(f"{tag}{i + 1}{k}", blk(b), rows(y), row, j)
        ring(f"ypf1{k}", blk(xm), rows(ym), row, yp)
        ring(f"ypf3{k}", ent(2 * x2), rows(ym), row, yp)
        ring(f"ymf2{k}", blk(xp), rows(yp), row, ym)
        ring(f"ymf3{k}", ent(2 * x2 + 1), rows(yp), row, ym)
    for k in range(SX):
        rows = (pl.ds(NY * SY + k % 2 * 2, 2), k // 2)
        ring(f"sp{k}", blk(x), rows, row_p, y)
        ring(f"sm{k}", blk(x), rows, row_m, y)
        ring(f"spf{k}", ent(2 * xm), rows, row_p, y)
        ring(f"smf{k}", ent(2 * xp + 1), rows, row_m, y)
    n_tile = NY * piece
    for k in range(EARLY):
        src = a_ref.at[pl.ds((SHIFT + k) * n_tile, n_tile)]
        there = ag_ref.at[x, pl.ds(k * n_tile, n_tile)]
        up = ag_ref.at[xm, pl.ds(k * n_tile, n_tile // 2)]
        down = ag_ref.at[xp, pl.ds(k * n_tile + n_tile // 2, n_tile // 2)]
        define(f"ap{k}", src, there, row_p, y)
        define(f"am{k}", src, there, row_m, y)
        define(f"apf{k}", up, up, row_p, y)
        define(f"amf{k}", down, down, row_m, y)

    regions = [(y * SY, SY), (NY * SY, SX)] + [(lax.rem(y + d, NY) * SY, SY) for d in range(1, NY)]
    local = []
    for s, (first, n) in enumerate(regions):
        there = xb.at[row, pl.ds(first, n)]
        local.append(pltpu.make_async_copy(x_ref.at[c, pl.ds(first, n)], there, loc.at[s]))
        define(f"d{s}", x_ref.at[1 - c, pl.ds(first, n)], there, partner, y)
    for d in range(1, n_ent):
        define(f"g{d}", g_ref, gb.at[row], lax.rem(row + d, n_ent), y)
    define("wg", wg_ref, wgb.at[c], partner, y)
    define("wu", wu_ref, wub.at[c], partner, y)
    local.append(pltpu.make_async_copy(g_ref, gb.at[row], loc.at[NY + 1]))
    local.append(pltpu.make_async_copy(wg_ref, wgb.at[c], loc.at[NY + 2]))
    local.append(pltpu.make_async_copy(wu_ref, wub.at[c], loc.at[NY + 3]))
    start(local)

    greet([(lax.rem(row + d, n_ent), y) for d in range(1, n_ent)] + [(row, yp), (row, ym)])

    copies["d0"].start()
    local[0].wait()
    start([copies["xp0a"], copies["xm0a"]])
    rest = [f"d{s}" for s in range(1, NY + 1)] + [f"g{d}" for d in range(1, n_ent)]
    start([copies[n] for n in rest + ["wg", "wu"]])
    got([copies["d0"]])
    start([copies["xp0b"], copies["xm0b"]])

    def act(tokens):
        for what, token in k1_steps(tokens):
            group, k = token[:-1], int(token[-1])
            if what == "s" and token == "s0":
                for s in range(1, NY + 1):
                    local[s].wait()
                    copies[f"d{s}"].wait_recv()
            for part in GROUPS[group]:
                for name in [f"{part}{k}a", f"{part}{k}b"] if token == "xp0" else [f"{part}{k}"]:
                    if what == "w":
                        copies[name].wait_recv()
                    elif token != "xp0":
                        copies[name].start()

    act(K1_PLAN[0])
    for cp in local[NY + 1 :]:
        cp.wait()
    got([copies[n] for n in [f"g{d}" for d in range(1, n_ent)] + ["wg", "wu"]])

    base = {"s": y * SY, "m": ym * SY, "p": yp * SY, "o": y2 * SY}

    def tile(s, _):
        for k in range(1, len(K1_TILES)):
            if K1_PLAN[k]:
                pl.when(s == k)(functools.partial(act, K1_PLAN[k]))
        pair, late, along = 0, 0, 0
        for k, name in enumerate(K1_TILES):
            i = int(name[1])
            where = (NY * SY + i % 2 * 2, i // 2, 1) if name[0] == "x" else (base[name[0]] + i, 0, 0)
            pair, late, along = (jnp.where(s == k, a, b) for a, b in zip(where, (pair, late, along)))
        pieces = [(pair, late), (pair + along, late + 1 - along)]

        for i, (p, t) in enumerate(pieces):

            def sixteen(g, _, p=p, t=t, i=i):
                r = pl.multiple_of(g * 16, 16)
                d = pl.multiple_of(i * piece + g * 16, 16)

                def store(e, v):
                    nt[pl.ds(d, 16), e * width : (e + 1) * width] = v

                norm_rows(lambda e: xb[e, p, t, pl.ds(r, 16), :], gb, 0, store, n_ent, width)
                return 0

            lax.fori_loop(0, piece // 16, sixteen, 0)

        step = min(256, ff)
        for h in range(2):
            for col in range(0, ff, step):
                gate = jnp.dot(nt[...], wgb[h, :, col : col + step], preferred_element_type=F32)
                up = jnp.dot(nt[...], wub[h, :, col : col + step], preferred_element_type=F32)
                act_val = (gate * lax.logistic(gate) * up).astype(BF16)
                for i, (p, t) in enumerate(pieces):
                    at = (p - lax.rem(p, NY)) * 2 + t * NY + lax.rem(p, NY)
                    r = pl.multiple_of(at * piece, 16)
                    a_ref[pl.ds(r, piece), h * ff + col : h * ff + col + step] = act_val[i * piece : (i + 1) * piece]
        return 0

    lax.fori_loop(0, len(K1_TILES), tile, 0)

    for q in range(CHUNKS):
        for t in range(2):
            for h in range(2):
                xres_ref[h, q, t] = xb[2 * x + h, NY * q + y, t]
    gout_ref[...] = gb[...]
    act(K1_PLAN[-1])
    for n in ids:
        copies[n].wait_send()


SEND = (5, 6, 6, 6, 6, 7, 9, 11)
PASS = (7, 8, 10, 9, 9, 8, 11, 11)
OUT = (3, 5, 8, 9)
RELAY = (5, 7, 10, 11)
QKV = (9, 11, 11, 11)
STEPS = 12
QKV_ORDER = tuple(sorted(range(CHUNKS), key=lambda n: (QKV[n], n)))

AP, AM, APF, AMF, S1L, S1R, FL, FR, GL, GR, XP, XM, XPF, XMF = range(14)
QPA, QPB, QMB, QMA, QPF, QMF, QD0, QD1, QD2, QD3A, QD3B, WD = range(12)
RP, RM, RPF, RMF, RD = 0, 2, 4, 5, 6


def k2(
    a_ref, ag_ref, wd_ref, xres_ref, gb_ref, wq_ref, resid_ref, out_ref,
    aall, wdb, pbuf, r1, rf, xg, wqb, nt, ob,
    send, recv, qsend, qrecv, rsend, rrecv, osend, orecv, loc, rloc, oloc,
):
    x, c, row, y = place()
    xp, xm, _ = around(x, NX)
    yp, ym, y2 = around(y, NY)
    n_ent = 2 * NX
    piece, width = pbuf.shape[3], pbuf.shape[4]
    rows_n = NY * piece
    ffc = a_ref.shape[1]
    qn = wq_ref.shape[0]
    row_p, row_m, partner = 2 * xp + c, 2 * xm + c, 2 * x + 1 - c

    def cols(i):
        return pl.ds(pl.multiple_of(i * ffc, 128), ffc)

    def at(i):
        return lax.rem(i + SHIFT, TILES)

    def chunk_of(n):
        return lax.rem(n + SHIFT // 2, CHUNKS)

    def rows(i, off=0, n=rows_n):
        return pl.ds(pl.multiple_of(at(i) * rows_n + off, 16), n)

    def wq_at(b, off=0, n=qn):
        return wqb.at[pl.ds(pl.multiple_of(b * qn + off, 16), n)]

    early_n = EARLY * rows_n
    cut = 2 * rows_n
    tail = pl.ds(SHIFT * rows_n, early_n)
    local = [
        pltpu.make_async_copy(a_ref.at[pl.ds(0, cut)], aall.at[pl.ds(0, cut), cols(x)], loc.at[0]),
        pltpu.make_async_copy(wd_ref, wdb.at[c], loc.at[1]),
        pltpu.make_async_copy(a_ref.at[pl.ds(cut, TILES * rows_n - cut)], aall.at[pl.ds(cut, TILES * rows_n - cut), cols(x)], loc.at[2]),
        pltpu.make_async_copy(wq_ref, wq_at(2 * y + c), loc.at[3]),
    ]
    for d in range(1, NX):
        other = lax.rem(x + d, NX)
        local.append(pltpu.make_async_copy(ag_ref.at[other], aall.at[tail, cols(other)], loc.at[3 + d]))
    start(local)

    column = [(2 * x + h, lax.rem(y + d, NY)) for d in range(1, NY) for h in range(2)]
    greet([(row_p, y), (row_m, y), (partner, y)] + column)

    def ring(kind, j, src, dst, to_row, to_y):
        return to(src, dst, send.at[kind, j], recv.at[kind, j], to_row, to_y)

    def own(i):
        ref = aall.at[rows(i), cols(x)]
        return ring(AP, i, ref, ref, row_p, y), ring(AM, i, ref, ref, row_m, y)

    def onward(i):
        h = rows_n // 2
        up, down = aall.at[rows(i, 0, h), cols(xm)], aall.at[rows(i, h, h), cols(xp)]
        return ring(APF, i, up, up, row_p, y), ring(AMF, i, down, down, row_m, y)

    def early(i):
        return (
            ring(S1L, i, pbuf.at[i, 0, y2], r1.at[i, 0], row, yp),
            ring(S1R, i, pbuf.at[i, 1, y2], r1.at[i, 1], row, ym),
            ring(FR, i, pbuf.at[i, 1, yp], rf.at[i, 1], row, yp),
            ring(GL, i, pbuf.at[i, 0, ym], rf.at[i, 2], row, ym),
        )

    def late(i):
        return (
            ring(FL, i, pbuf.at[i, 0, yp], rf.at[i, 0], row, yp),
            ring(GR, i, pbuf.at[i, 1, ym], rf.at[i, 3], row, ym),
        )

    def next_own(i):
        ref = xg.at[pl.ds(2 * x, 2), i]
        return ring(XP, i, ref, ref, row_p, y), ring(XM, i, ref, ref, row_m, y)

    def next_onward(i):
        up, down = xg.at[pl.ds(2 * xm, 1), i], xg.at[pl.ds(2 * xp + 1, 1), i]
        return ring(XPF, i, up, up, row_p, y), ring(XMF, i, down, down, row_m, y)

    def q(i, ref, to_row, to_y, src=None):
        return to(ref if src is None else src, ref, qsend.at[i], qrecv.at[i], to_row, to_y)

    n_a = (qn // 2 + 15) // 16 * 16
    n_b = qn - n_a
    mine, b_m, b_p, b_2 = 2 * y + c, 2 * ym + c, 2 * yp + c, 2 * y2 + c
    src_a, src_b = wq_ref.at[pl.ds(0, n_a)], wq_ref.at[pl.ds(n_a, n_b)]
    qs = {
        QPA: q(QPA, wq_at(mine, 0, n_a), row, yp, src_a),
        QPB: q(QPB, wq_at(mine, n_a, n_b), row, yp, src_b),
        QMB: q(QMB, wq_at(mine, n_a, n_b), row, ym, src_b),
        QMA: q(QMA, wq_at(mine, 0, n_a), row, ym, src_a),
        QPF: q(QPF, wq_at(b_m, 0, n_a), row, yp),
        QMF: q(QMF, wq_at(b_p, n_a, n_b), row, ym),
        QD0: q(QD0, wq_at(mine), partner, y, wq_ref),
        QD1: q(QD1, wq_at(b_m), partner, y),
        QD2: q(QD2, wq_at(b_p), partner, y),
        QD3A: q(QD3A, wq_at(b_2, 0, n_a), partner, y),
        QD3B: q(QD3B, wq_at(b_2, n_a, n_b), partner, y),
        WD: to(wd_ref, wdb.at[c], qsend.at[WD], qrecv.at[WD], partner, y),
    }

    def out(n):
        there = resid_ref.at[c, chunk_of(n), y]
        sends = []
        for h in range(2):
            src = xg.at[2 * x + h, pl.ds(2 * n, 2)]
            sends.append(to(src, there, rsend.at[RP + h, n], rrecv.at[RP + c, n], 2 * x + h, yp))
            sends.append(to(src, there, rsend.at[RM + h, n], rrecv.at[RM + c, n], 2 * x + h, ym))
        sends.append(to(xg.at[partner, pl.ds(2 * n, 2)], there, rsend.at[RD, n], rrecv.at[RD, n], partner, y))
        return sends

    def out_own(n):
        return pltpu.make_async_copy(xg.at[row, pl.ds(2 * n, 2)], resid_ref.at[c, chunk_of(n), y], rloc.at[n])

    def out_arrived(n):
        ref = resid_ref.at[0, chunk_of(n), y]
        return [to(xg.at[row, pl.ds(2 * n, 2)], ref, rsend.at[i, n], rrecv.at[i, n], row, yp) for i in range(4)]

    def relay(n):
        up, down = resid_ref.at[0, chunk_of(n), ym], resid_ref.at[1, chunk_of(n), yp]
        return (
            to(up, up, rsend.at[RPF, n], rrecv.at[RPF, n], row, yp),
            to(down, down, rsend.at[RMF, n], rrecv.at[RMF, n], row, ym),
        )

    def result(n, d, f):
        h = c if f == 0 else 1 - c
        to_y = lax.rem(y + d, NY)
        src = ob.at[n, 2 * to_y + h]
        first = (c * CHUNKS + chunk_of(n)) * NY + y
        dst = out_ref.at[:, pl.ds(pl.multiple_of(first * 2 * piece, 128), 2 * piece)]
        if d == 0 and f == 0:
            return pltpu.make_async_copy(src, dst, oloc.at[n])
        return to(src, dst, osend.at[n, 2 * d + f], orecv.at[n, 2 * d + f], 2 * x + h, to_y)

    def add_neighbour(i):
        got(early(i)[:2])
        for r in range(0, piece, 16):
            s = pl.ds(r, 16)
            pbuf[i, 0, yp, s, :] = pbuf[i, 0, yp, s, :] + r1[i, 0, s, :]
            pbuf[i, 1, ym, s, :] = pbuf[i, 1, ym, s, :] + r1[i, 1, s, :]
        start(late(i))

    def final(i):
        got(early(i)[2:] + late(i))
        for h in range(2):
            for r in range(0, piece, 16):
                s = pl.ds(r, 16)
                total = pbuf[i, h, y, s, :] + rf[i, h, s, :] + rf[i, 2 + h, s, :]
                held = xres_ref[h, lax.div(at(i), 2), lax.rem(i, 2), s, :].astype(F32)
                xg[2 * x + h, i, s, :] = (held + total).astype(BF16)

    def qkv(n):
        got(next_onward(2 * n) + next_onward(2 * n + 1))
        for t in range(2):

            def sixteen(g, _, t=t):
                r = pl.multiple_of(g * 16, 16)
                d = pl.multiple_of(t * piece + g * 16, 16)

                def store(e, v):
                    nt[pl.ds(d, 16), e * width : (e + 1) * width] = v

                norm_rows(lambda e: xg[e, 2 * n + t, pl.ds(r, 16), :], gb_ref, 1, store, n_ent, width)
                return 0

            lax.fori_loop(0, piece // 16, sixteen, 0)
        part = lax.dot_general(wqb[...], nt[...], (((1,), (1,)), ((), ())), preferred_element_type=F32)
        part = part.astype(BF16)
        for b in range(2 * NY):
            ob[n, b] = part[b * qn : (b + 1) * qn]
        for d in (2, 1, 3, 0):
            for f in range(2):
                result(n, d, f).start()

    def odd(i, lag):
        return lax.div(i - lag, 2)

    local[0].wait()
    start(own(EARLY))
    qs[WD].start()
    start(own(EARLY + 1))
    start([qs[i] for i in (QPA, QMB, QPB, QMA, QD0)])
    for cp in local[1:]:
        cp.wait()
    got([qs[WD]])

    step = min(256, width)

    def tile(i, _):
        @pl.when(i == 3)
        def _():
            got([qs[k] for k in (QPA, QMB, QPB, QMA)])
            start([qs[k] for k in (QPF, QMF, QD1, QD2)])

        @pl.when(i == 5)
        def _():
            got([qs[QPF], qs[QMF]])
            start([qs[QD3A], qs[QD3B]])

        @pl.when(i == 7)
        def _():
            got([qs[k] for k in (QD0, QD1, QD2, QD3A, QD3B)])

        @pl.when((i >= EARLY) & (i < TILES))
        def _():
            got(onward(i))

        @pl.when((i + 1 >= EARLY) & (i + 1 < TILES))
        def _():
            got(own(i + 1))
            start(onward(i + 1))

        @pl.when((i >= 1) & (i + EARLY + 1 < TILES))
        def _():
            start(own(i + EARLY + 1))

        @pl.when(i < TILES)
        def _():
            for h in range(2):
                for col in range(0, width, step):
                    part = jnp.dot(aall[rows(i), :], wdb[h, :, col : col + step], preferred_element_type=F32)
                    for k in range(NY):
                        pbuf[i, h, k, :, col : col + step] = part[k * piece : (k + 1) * piece]
            start(early(i))

        @pl.when((i >= 1) & (i <= TILES))
        def _():
            add_neighbour(i - 1)

        @pl.when((i >= 2) & (i <= TILES + 1))
        def _():
            final(i - 2)

        def extra(k):
            for j in range(TILES):
                if SEND[j] == k:
                    start(next_own(j))
            for n in range(CHUNKS):
                if OUT[n] == k:
                    start(out(n) + [out_own(n)])
            for j in range(TILES):
                if PASS[j] == k:
                    got(next_own(j))
                    start(next_onward(j))
            for n in range(CHUNKS):
                if RELAY[n] == k:
                    got(out_arrived(n))
                    start(relay(n))

        for k in sorted(set(SEND + PASS + OUT + RELAY)):
            pl.when(i == k)(functools.partial(extra, k))

        first, last = 0, 0
        for k in sorted(set(QKV)):
            first = jnp.where(i > k, sum(v <= k for v in QKV), first)
            last = jnp.where(i >= k, sum(v <= k for v in QKV), last)

        def chunk(m, _):
            n = QKV_ORDER[0]
            for k in range(1, CHUNKS):
                n = jnp.where(m == k, QKV_ORDER[k], n)
            qkv(n)
            return 0

        lax.fori_loop(first, last, chunk, 0)
        return 0

    lax.fori_loop(0, STEPS, tile, 0)

    def settle(i, _):
        for cp in early(i) + late(i) + next_own(i) + next_onward(i):
            cp.wait_send()

        @pl.when(i >= EARLY)
        def _():
            for cp in own(i) + onward(i):
                cp.wait_send()

        return 0

    lax.fori_loop(0, TILES, settle, 0)

    def settle_out(n, _):
        for cp in out(n) + list(relay(n)):
            cp.wait_send()
        got([out(n)[-1]] + list(relay(n)))
        out_own(n).wait()
        for d in range(NY):
            for f in range(2):
                result(n, d, f).wait()
        return 0

    lax.fori_loop(0, CHUNKS, settle_out, 0)
    for i in qs:
        qs[i].wait_send()


def solution(mesh):
    assert mesh.shape["row"] == 2 * NX and mesh.shape["col"] == NY
    tok_spec, gain_spec = P("data", "row"), P("row")
    wide_spec, down_spec, qkv_spec = P(None, ("col", "row")), P("col", "row"), P("data", ("col", "row"))

    def params(i):
        return pltpu.CompilerParams(collective_id=i, has_side_effects=True, vmem_limit_bytes=LIMIT)

    def per_device(residual, gain_mlp, gain_attn, w_gate, w_up, w_down, w_qkv):
        tokens, width = residual.shape
        hidden, ff = w_gate.shape
        qn = w_qkv.shape[1]
        half = tokens // 2
        piece = half // PAIRS // 2
        n_ent = 2 * NX
        gains = jnp.concatenate([gain_mlp[None], gain_attn[None], jnp.zeros((6, width), F32)])
        n1 = len(k1_names())
        act, xres, gb, ag = pl.pallas_call(
            k1,
            name="mlp_in",
            out_shape=[
                jax.ShapeDtypeStruct((half, 2 * ff), BF16),
                jax.ShapeDtypeStruct((2, CHUNKS, 2, piece, width), BF16),
                jax.ShapeDtypeStruct((n_ent, 8, width), F32),
                jax.ShapeDtypeStruct((NX, EARLY * NY * piece, 2 * ff), BF16),
            ],
            in_specs=[ANY] * 4,
            out_specs=[VMEM] * 3 + [ANY],
            scratch_shapes=[
                pltpu.VMEM((n_ent, PAIRS, 2, piece, width), BF16),
                pltpu.VMEM((2, hidden, ff), BF16),
                pltpu.VMEM((2, hidden, ff), BF16),
                pltpu.VMEM((2 * piece, hidden), BF16),
                pltpu.VMEM((n_ent, 8, width), F32),
                DMA((n1,)),
                DMA((n1,)),
                DMA((NY + 4,)),
            ],
            compiler_params=params(1),
        )(residual.reshape(2, PAIRS, 2, piece, width), gains, w_gate, w_up)
        resid, qkv_t = pl.pallas_call(
            k2,
            name="mlp_out_qkv",
            out_shape=[
                jax.ShapeDtypeStruct((2, CHUNKS, NY, 2, piece, width), BF16),
                jax.ShapeDtypeStruct((qn, tokens), BF16),
            ],
            in_specs=[ANY, ANY, ANY, VMEM, VMEM, ANY],
            out_specs=[ANY, ANY],
            scratch_shapes=[
                pltpu.VMEM((half, n_ent * ff), BF16),
                pltpu.VMEM((2, n_ent * ff, width), BF16),
                pltpu.VMEM((TILES, 2, NY, piece, width), F32),
                pltpu.VMEM((TILES, 2, piece, width), F32),
                pltpu.VMEM((TILES, 4, piece, width), F32),
                pltpu.VMEM((n_ent, TILES, piece, width), BF16),
                pltpu.VMEM((2 * NY * qn, hidden), BF16),
                pltpu.VMEM((2 * piece, hidden), BF16),
                pltpu.VMEM((CHUNKS, 2 * NY, qn, 2 * piece), BF16),
                DMA((14, TILES)),
                DMA((14, TILES)),
                DMA((12,)),
                DMA((12,)),
                DMA((7, CHUNKS)),
                DMA((7, CHUNKS)),
                DMA((CHUNKS, 2 * NY)),
                DMA((CHUNKS, 2 * NY)),
                DMA((7,)),
                DMA((CHUNKS,)),
                DMA((CHUNKS,)),
            ],
            compiler_params=params(2),
        )(act, ag, w_down, xres, gb, w_qkv.T)
        return resid.reshape(tokens, width), qkv_t.T

    return jax.shard_map(
        per_device,
        mesh=mesh,
        in_specs=(tok_spec, gain_spec, gain_spec, wide_spec, wide_spec, down_spec, wide_spec),
        out_specs=(tok_spec, qkv_spec),
        check_vma=False,
    )
```

```python
import functools

import jax
import jax.numpy as jnp
from jax import lax
from jax.experimental import pallas as pl
from jax.experimental.pallas import tpu as pltpu
from jax.sharding import PartitionSpec as P

NORM_EPS = 1e-6
MESH = pl.DeviceIdType.MESH
BF16 = jnp.bfloat16
F32 = jnp.float32
ANY = pl.BlockSpec(memory_space=pl.ANY)
VMEM = pl.BlockSpec(memory_space=pltpu.VMEM)
DMA = pltpu.SemaphoreType.DMA
LIMIT = 64 * 1024 * 1024 - 128 * 1024

NX, NY = 4, 4
PAIRS = 16
SY = 3
SX = PAIRS - NY * SY
TILES = PAIRS // 2
CHUNKS = TILES // 2
FIRST = NY * SY // 2
SLOTS = 4


def place():
    row, y = lax.axis_index("row"), lax.axis_index("col")
    return lax.div(row, 2), lax.rem(row, 2), row, y


def around(i, n):
    return lax.rem(i + 1, n), lax.rem(i + n - 1, n), lax.rem(i + 2, n)


def greet(peers):
    barrier = pltpu.get_barrier_semaphore()
    for row, y in peers:
        pl.semaphore_signal(barrier, inc=1, device_id={"row": row, "col": y}, device_id_type=MESH)
    pl.semaphore_wait(barrier, len(peers))


def to(src, dst, send, recv, row, y):
    return pltpu.make_async_remote_copy(src, dst, send, recv, device_id={"row": row, "col": y}, device_id_type=MESH)


def start(copies):
    for cp in copies:
        cp.start()


def got(copies):
    for cp in copies:
        cp.wait_recv()


def norm_rows(load, gains, store, n_ent, width):
    acc = None
    for e in range(n_ent):
        v = load(e).astype(F32)
        acc = v * v if acc is None else acc + v * v
    scale = lax.rsqrt(jnp.sum(acc, axis=1, keepdims=True) / (n_ent * width) + NORM_EPS)
    for e in range(n_ent):
        store(e, (load(e).astype(F32) * scale * gains[e]).astype(BF16))


def steps(tokens):
    out, what = [], None
    for token in tokens:
        if token in ("s", "w"):
            what = token
        else:
            out.append((what, token))
    return out


GROUPS = {
    "xp": ("xp", "xm"),
    "xf": ("xpf", "xmf"),
    "ya": ("yp1", "yp2", "ym1", "ym2"),
    "yb": ("yp3", "ym3"),
    "yf": ("ypf1", "ypf3", "ymf2", "ymf3"),
    "s": ("sp", "sm"),
    "sf": ("spf", "smf"),
}
COUNTS = {"xp": SY, "xf": SY, "ya": SY, "yb": SY, "yf": SY, "s": SX, "sf": SX}

IN_TILES = ("x0", "x1", "s0", "p0", "o0", "x2", "x3", "m0", "m1", "s2", "m2", "p1", "p2", "s1", "o1", "o2")
IN_PLAN = (
    ("s", "xp0", "s0", "w", "xp0", "s", "xf0", "w", "s0", "s", "sf0", "s1", "ya0", "xp2", "w", "s1", "s", "sf1", "s2", "xp1", "w", "xf0", "s", "yb0", "w", "xp2", "s", "ya2", "w", "s2", "s", "sf2", "w", "ya0", "yb0", "s", "yf0", "w", "sf0"),
    ("s", "s3", "w", "sf1"),
    (),
    ("w", "xp1", "s", "xf1", "w", "s3", "s", "sf3", "w", "xf1", "s", "yb1", "xf2", "a0", "ya1"),
    ("w", "yf0"),
    ("w", "sf2"),
    ("w", "sf3"),
    ("s", "a1", "w", "xf2", "s", "yb2"),
    ("w", "ya1", "yb1", "s", "yf1", "w", "a0", "s", "af0"),
    (),
    ("w", "ya2", "yb2", "s", "yf2", "q1", "a2"),
    (),
    (),
    (),
    ("w", "a1", "s", "af1", "w", "yf1"),
    ("w", "yf2"),
    ("s", "a3"),
)

ACT = (-1, -1, -1, -1, 1, 2, 3, 4)
SEND = (5, 6, 7, 6, 6, 7, 10, 9)
PASS = (7, 8, 7, 8, 9, 10, 11, 11)
OUT = (2, 4, 4, 5, 7, 8, 8, 9)
RELAY = (2, 4, 5, 5, 10, 11, 11, 11)
QKV = (9, 10, 11, 11)
Q_NEXT, Q_LAST, Q_LOAD = (0, 2, 4)
STEPS = 12
FIRST_S = next(n for n in IN_PLAN[0] if n[0] == "s" and n[1:].isdigit())
QKV_ORDER = tuple(sorted(range(CHUNKS), key=lambda n: (QKV[n], n)))
PASSED = tuple(sum(("s", f"af{i}") in steps(row) for row in IN_PLAN) for i in range(TILES))


def in_names():
    names = []
    for group, parts in GROUPS.items():
        for k in range(COUNTS[group]):
            for part in parts:
                names += [f"{part}{k}a", f"{part}{k}b"] if group == "xp" and k == 0 else [f"{part}{k}"]
    names += [f"d{d}{k}" for d in range(NY) for k in range(SY)] + [f"e{s}" for s in range(2 * SX)]
    names += [f"g{d}{k}" for d in range(1, 2 * NX) for k in range(2)]
    return names + ["wg", "wu", "wd"]


AP, AM, APF, AMF, S1L, S1R, FL, FR, GL, GR, XP, XM, XPF, XMF = range(14)
QPA, QPB, QMB, QMA, QPF, QMF, QD0, QD1, QD2, QD3A, QD3B = range(11)
RP, RM, RPF, RMF, RD = 0, 2, 4, 5, 6


def kernel(
    x_ref, g1_ref, g2_ref, wg_ref, wu_ref, wd_ref, wq_ref, resid_ref, out_ref, wdx_ref, wqa_ref,
    xb, wgb, wub, aall, pbuf, r1, rf, xres, nt, g1b, g2b, ob,
    isend, irecv, send, recv, qsend, qrecv, rsend, rrecv, osend, orecv, loc, rloc, oloc, ready,
):
    x, c, row, y = place()
    xp, xm, x2 = around(x, NX)
    yp, ym, y2 = around(y, NY)
    n_ent = 2 * NX
    width, ff, qn = xb.shape[2], wgb.shape[2], wq_ref.shape[0]
    piece = xb.shape[1] // (2 * PAIRS)
    pair_n, rows_n, ffc = 2 * piece, NY * piece, 2 * ff
    half = PAIRS * pair_n
    row_p, row_m, partner = 2 * xp + c, 2 * xm + c, 2 * x + 1 - c
    ids = {n: i for i, n in enumerate(in_names())}
    copies = {}


    def define(name, src, dst, to_row, to_y):
        i = ids[name]
        copies[name] = to(src, dst, isend.at[i], irecv.at[i], to_row, to_y)

    def circle(name, ents, where, to_row, to_y):
        ref = xb.at[ents, where]
        define(name, ref, ref, to_row, to_y)

    def span(first, n):
        return pl.ds(pl.multiple_of(first * piece, piece), n * piece)

    blk = lambda i: pl.ds(2 * i, 2)
    ent = lambda i: pl.ds(i, 1)
    for k in range(SY):
        where = lambda j: span(2 * (NY * k + j), 2)
        for part, j in (("xp", row_p), ("xm", row_m)):
            if k == 0:
                circle(f"{part}0a", ent(row), where(y), j, y)
                circle(f"{part}0b", ent(partner), where(y), j, y)
            else:
                circle(f"{part}{k}", blk(x), where(y), j, y)
        circle(f"xpf{k}", ent(2 * xm), where(y), row_p, y)
        circle(f"xmf{k}", ent(2 * xp + 1), where(y), row_m, y)
        for tag, j in (("yp", yp), ("ym", ym)):
            for i, b in enumerate((xm, xp, x2)):
                circle(f"{tag}{i + 1}{k}", blk(b), where(y), row, j)
        circle(f"ypf1{k}", blk(xm), where(ym), row, yp)
        circle(f"ypf3{k}", ent(2 * x2), where(ym), row, yp)
        circle(f"ymf2{k}", blk(xp), where(yp), row, ym)
        circle(f"ymf3{k}", ent(2 * x2 + 1), where(yp), row, ym)
    for k in range(SX):
        where = pl.ds((2 * NY * SY + 2 * k) * piece, 2 * piece)
        circle(f"sp{k}", blk(x), where, row_p, y)
        circle(f"sm{k}", blk(x), where, row_m, y)
        circle(f"spf{k}", ent(2 * xm), where, row_p, y)
        circle(f"smf{k}", ent(2 * xp + 1), where, row_m, y)

    local = {}

    def bring(name, i, src_at, dst_at, n):
        there = xb.at[row, span(dst_at, n)]
        mine = pl.ds(pl.multiple_of(c * half + src_at * piece, piece), n * piece)
        theirs = pl.ds(pl.multiple_of((1 - c) * half + src_at * piece, piece), n * piece)
        local[name] = pltpu.make_async_copy(x_ref.at[mine], there, loc.at[i])
        define(name, x_ref.at[theirs], there, partner, y)

    for d in range(NY):
        j = lax.rem(y + d, NY)
        for k in range(SY):
            bring(f"d{d}{k}", d * SY + k, 2 * (NY * k + j), 2 * (NY * k + j), 2)
    for k in range(2 * SX):
        t, p = k // SX, k % SX
        bring(f"e{k}", NY * SY + k, 2 * (NY * SY + p) + t, 2 * NY * SY + k, 1)
    n_loc = NY * SY + 2 * SX
    for d in range(1, n_ent):
        define(f"g{d}0", g1_ref, g1b.at[row], lax.rem(row + d, n_ent), y)
        define(f"g{d}1", g2_ref, g2b.at[row], lax.rem(row + d, n_ent), y)
    define("wg", wg_ref, wgb.at[c], partner, y)
    define("wu", wu_ref, wub.at[c], partner, y)
    define("wd", wd_ref, wdx_ref, partner, y)
    weights = [
        pltpu.make_async_copy(g1_ref, g1b.at[row], loc.at[n_loc]),
        pltpu.make_async_copy(wg_ref, wgb.at[c], loc.at[n_loc + 1]),
        pltpu.make_async_copy(wu_ref, wub.at[c], loc.at[n_loc + 2]),
        pltpu.make_async_copy(g2_ref, g2b.at[row], loc.at[n_loc + 3]),
    ]
    start(local.values())
    start(weights)

    greet(
        [(lax.rem(row + d, n_ent), y) for d in range(1, n_ent)]
        + [(2 * x + h, lax.rem(y + d, NY)) for d in range(1, NY) for h in range(2)]
    )

    copies["d00"].start()
    local["d00"].wait()
    start([copies["xp0a"], copies["xm0a"]])
    own_rows = [f"d0{k}" for k in range(1, SY)]
    round_x = [n for n in local if n[0] == "e"]
    other_rows = [n for n in local if n[0] == "d" and n[1] != "0"]
    start([copies[n] for n in own_rows + round_x])
    start([copies[n] for n in other_rows + [f"g{d}{k}" for d in range(1, n_ent) for k in range(2)] + ["wg", "wu", "wd"]])

    def q(i, ref, to_row, to_y, src=None):
        return to(ref if src is None else src, ref, qsend.at[i], qrecv.at[i], to_row, to_y)

    def wq_at(b, off=0, n=qn):
        return wqa_ref.at[pl.ds(pl.multiple_of(b * qn + off, 16), n)]

    n_a = (qn // 2 + 15) // 16 * 16
    n_b = qn - n_a
    mine, b_m, b_p, b_2 = 2 * y + c, 2 * ym + c, 2 * yp + c, 2 * y2 + c
    src_a, src_b = wq_ref.at[pl.ds(0, n_a)], wq_ref.at[pl.ds(n_a, n_b)]
    qs = {
        QPA: q(QPA, wq_at(mine, 0, n_a), row, yp, src_a),
        QPB: q(QPB, wq_at(mine, n_a, n_b), row, yp, src_b),
        QMB: q(QMB, wq_at(mine, n_a, n_b), row, ym, src_b),
        QMA: q(QMA, wq_at(mine, 0, n_a), row, ym, src_a),
        QPF: q(QPF, wq_at(b_m, 0, n_a), row, yp),
        QMF: q(QMF, wq_at(b_p, n_a, n_b), row, ym),
        QD0: q(QD0, wq_at(mine), partner, y, wq_ref),
        QD1: q(QD1, wq_at(b_m), partner, y),
        QD2: q(QD2, wq_at(b_p), partner, y),
        QD3A: q(QD3A, wq_at(b_2, 0, n_a), partner, y),
        QD3B: q(QD3B, wq_at(b_2, n_a, n_b), partner, y),
    }
    start([qs[QPA], qs[QMB], qs[QD0]])
    got([copies["d00"]])
    start([copies["xp0b"], copies["xm0b"]])
    for n in own_rows:
        local[n].wait()
    got([copies[n] for n in own_rows])
    weights[0].wait()
    for first in range(0, qn, nt.shape[0]):
        n = min(nt.shape[0], qn - first)
        for a, b in ((wq_ref.at[pl.ds(first, n)], nt.at[pl.ds(0, n)]), (nt.at[pl.ds(0, n)], wq_at(mine, first, n))):
            cp = pltpu.make_async_copy(a, b, loc.at[n_loc])
            cp.start()
            cp.wait()

    def cols(i):
        return pl.ds(pl.multiple_of(i * ffc, 128), ffc)

    def at(i):
        return lax.rem(i + FIRST, TILES)

    def chunk_of(n):
        return lax.rem(n + FIRST // 2, CHUNKS)

    def rows(i, off=0, n=rows_n):
        return pl.ds(pl.multiple_of(at(i) * rows_n + off, 16), n)

    def ring(kind, j, src, dst, to_row, to_y):
        return to(src, dst, send.at[kind, j], recv.at[kind, j], to_row, to_y)

    def own(i):
        ref = aall.at[rows(i), cols(x)]
        return ring(AP, i, ref, ref, row_p, y), ring(AM, i, ref, ref, row_m, y)

    def onward(i):
        h = rows_n // 2
        up, down = aall.at[rows(i, 0, h), cols(xm)], aall.at[rows(i, h, h), cols(xp)]
        return ring(APF, i, up, up, row_p, y), ring(AMF, i, down, down, row_m, y)

    def act(tokens):
        for what, token in steps(tokens):
            group, k = token[:-1], int(token[-1])
            if what == "s" and token == FIRST_S:
                for n in round_x:
                    local[n].wait()
                got([copies[n] for n in round_x])
            if group == "q":
                cps = [qs[QPB], qs[QMA]]
            elif group in ("a", "af"):
                cps = own(k) if group == "a" else onward(k)
            else:
                cps = []
                for part in GROUPS[group]:
                    cps += [copies[n] for n in ([f"{part}0a", f"{part}0b"] if token == "xp0" else [f"{part}{k}"])]
            if what == "w":
                got(cps)
            elif token != "xp0":
                start(cps)

    act(IN_PLAN[0])
    for cp in [local[n] for n in other_rows] + weights[1:]:
        cp.wait()
    got([copies[n] for n in other_rows])
    got([copies[n] for n in [f"g{d}{k}" for d in range(1, n_ent) for k in range(2)] + ["wg", "wu"]])

    base = {"s": y, "m": ym, "p": yp, "o": y2}

    def in_tile(s, _):
        for k in range(1, len(IN_TILES)):
            if IN_PLAN[k]:
                pl.when(s == k)(functools.partial(act, IN_PLAN[k]))
        first, p0, p1 = 0, 0, 0
        for k, name in enumerate(IN_TILES):
            i = int(name[1])
            if name[0] == "x":
                where = (2 * NY * SY + 2 * i, 2 * NY * SY + 2 * i, 2 * NY * SY + 2 * i + 1)
            else:
                j = base[name[0]]
                where = (2 * (NY * i + j), 2 * NY * i + j, 2 * NY * i + NY + j)
            first, p0, p1 = (jnp.where(s == k, a, b) for a, b in zip(where, (first, p0, p1)))

        def sixteen(g, _):
            r = pl.multiple_of(first * piece + g * 16, 16)
            d = pl.multiple_of(g * 16, 16)

            def store(e, v):
                nt[pl.ds(d, 16), e * width : (e + 1) * width] = v

            norm_rows(lambda e: xb[e, pl.ds(r, 16), :], g1b, store, n_ent, width)
            return 0

        lax.fori_loop(0, pair_n // 16, sixteen, 0)

        step = min(256, ff)
        for h in range(2):
            for col in range(0, ff, step):
                gate = jnp.dot(nt[...], wgb[h, :, col : col + step], preferred_element_type=F32)
                up = jnp.dot(nt[...], wub[h, :, col : col + step], preferred_element_type=F32)
                act_val = (gate * lax.logistic(gate) * up).astype(BF16)
                there = pl.ds(pl.multiple_of(x * ffc + h * ff + col, 128), step)
                for i, p in enumerate((p0, p1)):
                    aall[pl.ds(pl.multiple_of(p * piece, piece), piece), there] = act_val[i * piece : (i + 1) * piece]
        return 0

    lax.fori_loop(0, len(IN_TILES), in_tile, 0)
    act(IN_PLAN[-1])


    got([copies["wd"]])
    down = [
        pltpu.make_async_copy(wd_ref, wgb.at[c], loc.at[0]),
        pltpu.make_async_copy(wdx_ref, wgb.at[1 - c], loc.at[1]),
    ]
    start(down)
    for j in (row_p, row_m):
        pl.semaphore_signal(ready, inc=1, device_id={"row": j, "col": y}, device_id_type=MESH)
    for i in range(TILES):
        q_at, t = (i + FIRST) % TILES // 2, i % 2
        if q_at * NY < NY * SY:
            first = 2 * (NY * q_at + y) + t
        else:
            first = 2 * NY * SY + t * SX + y
        for h in range(2):
            xres[h, i] = xb[2 * x + h, span(first, 1), :]
    for n in ids:
        copies[n].wait_send()
    for cp in down:
        cp.wait()
    pl.semaphore_wait(ready, 2)


    def early(i):
        slot = lax.rem(i, SLOTS)
        return (
            ring(S1L, i, pbuf.at[slot, 0, y2], r1.at[i, 0], row, yp),
            ring(S1R, i, pbuf.at[slot, 1, y2], r1.at[i, 1], row, ym),
            ring(FR, i, pbuf.at[slot, 1, yp], rf.at[i, 1], row, yp),
            ring(GL, i, pbuf.at[slot, 0, ym], rf.at[i, 2], row, ym),
        )

    def late(i):
        slot = lax.rem(i, SLOTS)
        return (
            ring(FL, i, pbuf.at[slot, 0, yp], rf.at[i, 0], row, yp),
            ring(GR, i, pbuf.at[slot, 1, ym], rf.at[i, 3], row, ym),
        )

    def held(i, e, n=1):
        return wub.at[0, pl.ds(pl.multiple_of((i * n_ent + e) * piece, piece), n * piece)]

    def next_own(i):
        ref = held(i, 2 * x, 2)
        return ring(XP, i, ref, ref, row_p, y), ring(XM, i, ref, ref, row_m, y)

    def next_onward(i):
        up, down = held(i, 2 * xm), held(i, 2 * xp + 1)
        return ring(XPF, i, up, up, row_p, y), ring(XMF, i, down, down, row_m, y)

    def home(i, of_c, of_y):
        return resid_ref.at[of_c, lax.div(at(i), 2), of_y, lax.rem(i, 2)]

    def out(i):
        there = home(i, c, y)
        sends = []
        for h in range(2):
            src = held(i, 2 * x + h)
            sends.append(to(src, there, rsend.at[RP + h, i], rrecv.at[RP + c, i], 2 * x + h, yp))
            sends.append(to(src, there, rsend.at[RM + h, i], rrecv.at[RM + c, i], 2 * x + h, ym))
        sends.append(to(held(i, partner), there, rsend.at[RD, i], rrecv.at[RD, i], partner, y))
        return sends

    def out_own(i):
        return pltpu.make_async_copy(held(i, row), home(i, c, y), rloc.at[i])

    def out_arrived(i):
        return [to(held(i, row), home(i, 0, y), rsend.at[k, i], rrecv.at[k, i], row, yp) for k in range(4)]

    def relay(i):
        up, down = home(i, 0, ym), home(i, 1, yp)
        return (
            to(up, up, rsend.at[RPF, i], rrecv.at[RPF, i], row, yp),
            to(down, down, rsend.at[RMF, i], rrecv.at[RMF, i], row, ym),
        )

    def result(n, d, f):
        h = c if f == 0 else 1 - c
        to_y = lax.rem(y + d, NY)
        src = ob.at[n, 2 * to_y + h]
        first = (c * CHUNKS + chunk_of(n)) * NY + y
        dst = out_ref.at[:, pl.ds(pl.multiple_of(first * pair_n, 128), pair_n)]
        if d == 0 and f == 0:
            return pltpu.make_async_copy(src, dst, oloc.at[n])
        return to(src, dst, osend.at[n, 2 * d + f], orecv.at[n, 2 * d + f], 2 * x + h, to_y)

    def add_neighbour(i):
        got(early(i)[:2])
        slot = lax.rem(i, SLOTS)
        for r in range(0, piece, 16):
            s = pl.ds(r, 16)
            pbuf[slot, 0, yp, s, :] = pbuf[slot, 0, yp, s, :] + r1[i, 0, s, :]
            pbuf[slot, 1, ym, s, :] = pbuf[slot, 1, ym, s, :] + r1[i, 1, s, :]
        start(late(i))

    def final(i):
        got(early(i)[2:] + late(i))
        slot = lax.rem(i, SLOTS)
        for h in range(2):
            ref = held(i, 2 * x + h)
            for r in range(0, piece, 16):
                s = pl.ds(r, 16)
                total = pbuf[slot, h, y, s, :] + rf[i, h, s, :] + rf[i, 2 + h, s, :]
                ref[s, :] = (xres[h, i, s, :].astype(F32) + total).astype(BF16)

    def qkv(n):
        got(next_onward(2 * n) + next_onward(2 * n + 1))
        for t in range(2):

            def sixteen(g, _, t=t):
                r = pl.multiple_of(g * 16, 16)
                d = pl.multiple_of(t * piece + g * 16, 16)

                def store(e, v):
                    nt[pl.ds(d, 16), e * width : (e + 1) * width] = v

                norm_rows(lambda e: held(2 * n + t, e)[pl.ds(r, 16), :], g2b, store, n_ent, width)
                return 0

            lax.fori_loop(0, piece // 16, sixteen, 0)
        for b in range(0, 2 * NY, 2):
            part = None
            for e in range(n_ent):
                lhs, rhs = xb[e, b * qn : (b + 2) * qn, :], nt[:, e * width : (e + 1) * width]
                term = lax.dot_general(lhs, rhs, (((1,), (1,)), ((), ())), preferred_element_type=F32)
                part = term if part is None else part + term
            part = part.astype(BF16)
            for k in range(2):
                ob[n, b + k] = part[k * qn : (k + 1) * qn]
        for d in (2, 1, 3, 0):
            for f in range(2):
                result(n, d, f).start()

    def wq_load(e):
        src = wqa_ref.at[:, pl.ds(e * width, width)]
        return pltpu.make_async_copy(src, xb.at[e, pl.ds(0, 2 * NY * qn)], loc.at[e])

    step = min(256, width)

    def tile(i, _):
        @pl.when(i == Q_NEXT)
        def _():
            got([qs[k] for k in (QPA, QMB, QPB, QMA)])
            start([qs[k] for k in (QPF, QMF, QD1, QD2)])

        @pl.when(i == Q_LAST)
        def _():
            got([qs[QPF], qs[QMF]])
            start([qs[QD3A], qs[QD3B]])

        @pl.when(i == Q_LOAD)
        def _():
            got([qs[k] for k in (QD0, QD1, QD2, QD3A, QD3B)])
            start([wq_load(e) for e in range(n_ent)])

        @pl.when(i == Q_LOAD + 1)
        def _():
            for e in range(n_ent):
                wq_load(e).wait()

        @pl.when(i < TILES)
        def _():
            got(onward(i))

        @pl.when((i + 1 >= sum(PASSED)) & (i + 1 < TILES))
        def _():
            got(own(i + 1))
            start(onward(i + 1))

        for k in sorted(set(ACT)):
            if k >= 0:
                pl.when(i == k)(lambda k=k: [start(own(j)) for j in range(TILES) if ACT[j] == k] and None)

        @pl.when((i >= SLOTS) & (i < TILES))
        def _():
            for cp in early(i - SLOTS) + late(i - SLOTS):
                cp.wait_send()

        @pl.when(i < TILES)
        def _():
            slot = lax.rem(i, SLOTS)
            for h in range(2):
                for col in range(0, width, step):
                    part = jnp.dot(aall[rows(i), :], wgb[h, :, col : col + step], preferred_element_type=F32)
                    for k in range(NY):
                        pbuf[slot, h, k, :, col : col + step] = part[k * piece : (k + 1) * piece]
            start(early(i))

        @pl.when((i >= 1) & (i <= TILES))
        def _():
            add_neighbour(i - 1)

        @pl.when((i >= 2) & (i <= TILES + 1))
        def _():
            final(i - 2)

        def extra(k):
            for j in range(TILES):
                if SEND[j] == k:
                    start(next_own(j))
            for j in range(TILES):
                if OUT[j] == k:
                    start(out(j) + [out_own(j)])
            for j in range(TILES):
                if PASS[j] == k:
                    got(next_own(j))
                    start(next_onward(j))
            for j in range(TILES):
                if RELAY[j] == k:
                    got(out_arrived(j))
                    start(relay(j))

        for k in sorted(set(SEND + PASS + OUT + RELAY)):
            pl.when(i == k)(functools.partial(extra, k))

        first, last = 0, 0
        for k in sorted(set(QKV)):
            first = jnp.where(i > k, sum(v <= k for v in QKV), first)
            last = jnp.where(i >= k, sum(v <= k for v in QKV), last)

        def chunk(m, _):
            n = QKV_ORDER[0]
            for k in range(1, CHUNKS):
                n = jnp.where(m == k, QKV_ORDER[k], n)
            qkv(n)
            return 0

        lax.fori_loop(first, last, chunk, 0)
        return 0

    lax.fori_loop(0, STEPS, tile, 0)

    def settle(i, _):
        for cp in own(i) + onward(i) + next_own(i) + next_onward(i):
            cp.wait_send()
        for cp in out(i) + list(relay(i)):
            cp.wait_send()
        got([out(i)[-1]] + list(relay(i)))
        out_own(i).wait()

        @pl.when(i >= TILES - SLOTS)
        def _():
            for cp in early(i) + late(i):
                cp.wait_send()

        return 0

    lax.fori_loop(0, TILES, settle, 0)

    def settle_out(n, _):
        for d in range(NY):
            for f in range(2):
                result(n, d, f).wait()
        return 0

    lax.fori_loop(0, CHUNKS, settle_out, 0)
    for i in qs:
        qs[i].wait_send()


def hand_over(a_ref, b_ref, a_out, b_out, a_buf, b_buf, a_in_sem, a_out_sem, b_sem):
    n = a_in_sem.shape[0]
    rows = a_ref.shape[0] // n
    part = lambda ref, i: ref.at[pl.ds(i * rows, rows)]
    ins = [pltpu.make_async_copy(part(a_ref, i), part(a_buf, i), a_in_sem.at[i]) for i in range(n)]
    outs = [pltpu.make_async_copy(part(a_buf, i), part(a_out, i), a_out_sem.at[i]) for i in range(n)]
    b_in = pltpu.make_async_copy(b_ref, b_buf, b_sem.at[0])
    b_back = pltpu.make_async_copy(b_buf, b_out, b_sem.at[1])
    start(ins + [b_in])
    for i in range(n):
        ins[i].wait()
        outs[i].start()
    b_in.wait()
    b_back.start()
    for cp in outs + [b_back]:
        cp.wait()


def solution(mesh):
    assert mesh.shape["row"] == 2 * NX and mesh.shape["col"] == NY
    tok_spec, gain_spec = P("data", "row"), P("row")
    wide_spec, down_spec, qkv_spec = P(None, ("col", "row")), P("col", "row"), P("data", ("col", "row"))

    def per_device(residual, gain_mlp, gain_attn, w_gate, w_up, w_down, w_qkv):
        tokens, width = residual.shape
        hidden, ff = w_gate.shape
        qn = w_qkv.shape[1]
        half = tokens // 2
        piece = half // PAIRS // 2
        n_ent = 2 * NX
        n_in = len(in_names())
        resid, qkv_t, _, _ = pl.pallas_call(
            kernel,
            name="mlp_qkv",
            out_shape=[
                jax.ShapeDtypeStruct((2, CHUNKS, NY, 2, piece, width), BF16),
                jax.ShapeDtypeStruct((qn, tokens), BF16),
                jax.ShapeDtypeStruct((n_ent * ff, width), BF16),
                jax.ShapeDtypeStruct((2 * NY * qn, hidden), BF16),
            ],
            in_specs=[ANY] * 7,
            out_specs=[ANY] * 4,
            scratch_shapes=[
                pltpu.VMEM((n_ent, half, width), BF16),
                pltpu.VMEM((2, hidden, ff), BF16),
                pltpu.VMEM((2, hidden, ff), BF16),
                pltpu.VMEM((half, n_ent * ff), BF16),
                pltpu.VMEM((SLOTS, 2, NY, piece, width), F32),
                pltpu.VMEM((TILES, 2, piece, width), F32),
                pltpu.VMEM((TILES, 4, piece, width), F32),
                pltpu.VMEM((2, TILES, piece, width), BF16),
                pltpu.VMEM((2 * piece, hidden), BF16),
                pltpu.VMEM((n_ent, 1, width), F32),
                pltpu.VMEM((n_ent, 1, width), F32),
                pltpu.VMEM((CHUNKS, 2 * NY, qn, 2 * piece), BF16),
                DMA((n_in,)),
                DMA((n_in,)),
                DMA((14, TILES)),
                DMA((14, TILES)),
                DMA((11,)),
                DMA((11,)),
                DMA((7, TILES)),
                DMA((7, TILES)),
                DMA((CHUNKS, 2 * NY)),
                DMA((CHUNKS, 2 * NY)),
                DMA((NY * SY + 2 * SX + 4,)),
                DMA((TILES,)),
                DMA((CHUNKS,)),
                pltpu.SemaphoreType.REGULAR,
            ],
            compiler_params=pltpu.CompilerParams(collective_id=1, has_side_effects=True, vmem_limit_bytes=LIMIT),
        )(residual, gain_mlp[None], gain_attn[None], w_gate, w_up, w_down, w_qkv.T)
        parts = 8
        resid, qkv_t = pl.pallas_call(
            hand_over,
            name="hand_over",
            out_shape=[jax.ShapeDtypeStruct((tokens, width), BF16), jax.ShapeDtypeStruct((qn, tokens), BF16)],
            in_specs=[ANY] * 2,
            out_specs=[ANY] * 2,
            scratch_shapes=[
                pltpu.VMEM((tokens, width), BF16),
                pltpu.VMEM((qn, tokens), BF16),
                DMA((parts,)),
                DMA((parts,)),
                DMA((2,)),
            ],
        )(resid.reshape(tokens, width), qkv_t)
        return resid, qkv_t.T

    return jax.shard_map(
        per_device,
        mesh=mesh,
        in_specs=(tok_spec, gain_spec, gain_spec, wide_spec, wide_spec, down_spec, wide_spec),
        out_specs=(tok_spec, qkv_spec),
        check_vma=False,
    )
```

```python
import functools

import jax
import jax.numpy as jnp
from jax import lax
from jax.experimental import pallas as pl
from jax.experimental.pallas import tpu as pltpu
from jax.sharding import PartitionSpec as P

NORM_EPS = 1e-6
MESH = pl.DeviceIdType.MESH
BF16 = jnp.bfloat16
F32 = jnp.float32
ANY = pl.BlockSpec(memory_space=pl.ANY)
VMEM = pl.BlockSpec(memory_space=pltpu.VMEM)
DMA = pltpu.SemaphoreType.DMA
LIMIT = 64 * 1024 * 1024 - 128 * 1024

NX, NY = 4, 4
PAIRS = 16
SY = 3
SX = PAIRS - NY * SY
TILES = PAIRS // 2
CHUNKS = TILES // 2
FIRST = NY * SY // 2
SLOTS = 4


def place():
    row, y = lax.axis_index("row"), lax.axis_index("col")
    return lax.div(row, 2), lax.rem(row, 2), row, y


def around(i, n):
    return lax.rem(i + 1, n), lax.rem(i + n - 1, n), lax.rem(i + 2, n)


def greet(peers):
    barrier = pltpu.get_barrier_semaphore()
    for row, y in peers:
        pl.semaphore_signal(barrier, inc=1, device_id={"row": row, "col": y}, device_id_type=MESH)
    pl.semaphore_wait(barrier, len(peers))


def to(src, dst, send, recv, row, y):
    return pltpu.make_async_remote_copy(src, dst, send, recv, device_id={"row": row, "col": y}, device_id_type=MESH)


def start(copies):
    for cp in copies:
        cp.start()


def got(copies):
    for cp in copies:
        cp.wait_recv()


def norm_rows(load, gains, store, n_ent, width):
    acc = None
    for e in range(n_ent):
        v = load(e).astype(F32)
        acc = v * v if acc is None else acc + v * v
    scale = lax.rsqrt(jnp.sum(acc, axis=1, keepdims=True) / (n_ent * width) + NORM_EPS)
    for e in range(n_ent):
        store(e, (load(e).astype(F32) * scale * gains[e]).astype(BF16))


def steps(tokens):
    out, what = [], None
    for token in tokens:
        if token in ("s", "w"):
            what = token
        else:
            out.append((what, token))
    return out


GROUPS = {
    "xp": ("xp", "xm"),
    "xf": ("xpf", "xmf"),
    "ya": ("yp1", "yp2", "ym1", "ym2"),
    "yb": ("yp3", "ym3"),
    "yf": ("ypf1", "ypf3", "ymf2", "ymf3"),
    "s": ("sp", "sm"),
    "sf": ("spf", "smf"),
}
COUNTS = {"xp": SY, "xf": SY, "ya": SY, "yb": SY, "yf": SY, "s": SX, "sf": SX}

IN_TILES = ("p0", "m0", "s0", "o0", "s1", "x1", "x0", "x2", "x3", "s2", "m1", "o1", "m2", "p1", "p2", "o2")
IN_PLAN = (
    ("s", "xp0", "s2", "xp1", "w", "xp0", "s", "xf0", "s1", "ya0", "w", "xp1", "s", "xf1", "w", "xf0", "s", "yb0", "s3", "w", "ya0", "yb0", "s", "yf0", "w", "s1", "s", "sf1", "xp2"),
    (),
    ("s", "ya1", "w", "s2", "s", "sf2", "s0", "w", "xp2", "s", "xf2", "w", "s3", "s", "sf3"),
    ("w", "yf0"),
    ("s", "ya2", "w", "xf1"),
    ("s", "a3", "w", "sf1"),
    ("w", "s0", "s", "sf0", "w", "xf2", "s", "yb2", "yb1", "a2", "w", "sf0"),
    ("w", "ya1", "yb1", "s", "yf1", "w", "a3", "s", "af3", "w", "sf2"),
    ("w", "sf3"),
    ("s", "a1", "q1", "a0"),
    ("w", "ya2", "yb2", "s", "yf2"),
    ("w", "yf1"),
    (),
    (),
    (),
    ("w", "a1", "s", "af1", "w", "a2", "s", "af2", "q2", "w", "a0", "s", "af0", "w", "yf2"),
    (),
)

HEAVY = (
    ("mm", 1),
    ("mm", 3),
    ("add", 3),
    ("add", 1),
    ("mm", 0),
    ("mm", 2),
    ("fin", 1),
    ("fin", 3),
    ("add", 0),
    ("add", 2),
    ("fin", 0),
    ("mm", 5),
    ("fin", 2),
    ("add", 5),
    ("fin", 5),
    ("mm", 4),
    ("add", 4),
    ("mm", 6),
    ("fin", 4),
    ("add", 6),
    ("mm", 7),
    ("fin", 6),
    ("add", 7),
    ("fin", 7),
    ("qkv", 2),
    ("qkv", 1),
    ("qkv", 0),
    ("qkv", 3),
)
LIGHT = (
    ("a5",),
    ("a4",),
    (),
    (),
    (),
    (),
    ("q3", "af5"),
    ("a6",),
    (),
    (),
    ("out1",),
    ("out0",),
    ("relay1", "af4"),
    (),
    ("out3", "af6"),
    ("out5", "a7", "relay0"),
    ("send5",),
    (),
    (),
    ("out2", "af7", "send4", "send2", "out4", "relay2"),
    ("q4", "send3"),
    ("pass4", "pass5", "send1"),
    ("send0", "out6"),
    ("relay4", "pass2", "relay3", "relay6", "send6"),
    ("relay5", "pass3", "pass0", "send7", "out7", "pass1", "q5"),
    (),
    ("relay7", "pass7", "pass6"),
    (),
)
KINDS = ("mm", "add", "fin", "qkv")
FIRST_S = next(n for n in IN_PLAN[0] if n[0] == "s" and n[1:].isdigit())


def in_names():
    names = []
    for group, parts in GROUPS.items():
        for k in range(COUNTS[group]):
            for part in parts:
                names += [f"{part}{k}a", f"{part}{k}b"] if group == "xp" and k == 0 else [f"{part}{k}"]
    names += [f"d{d}{k}" for d in range(NY) for k in range(SY)] + [f"e{s}" for s in range(2 * SX)]
    names += [f"g{d}{k}" for d in range(1, 2 * NX) for k in range(2)]
    return names + ["wg", "wu", "wd"]


AP, AM, APF, AMF, S1L, S1R, FL, FR, GL, GR, XP, XM, XPF, XMF = range(14)
QPA, QPB, QMB, QMA, QPF, QMF, QD0, QD1, QD2, QD3A, QD3B = range(11)
RP, RM, RPF, RMF, RD = 0, 2, 4, 5, 6


def kernel(
    x_ref, g1_ref, g2_ref, wg_ref, wu_ref, wd_ref, wq_ref, resid_ref, out_ref, wdx_ref, wqa_ref,
    xb, wgb, wub, aall, pbuf, r1, rf, xres, nt, g1b, g2b, ob,
    isend, irecv, send, recv, qsend, qrecv, rsend, rrecv, osend, orecv, loc, rloc, oloc, ready,
):
    x, c, row, y = place()
    xp, xm, x2 = around(x, NX)
    yp, ym, y2 = around(y, NY)
    n_ent = 2 * NX
    width, ff, qn = xb.shape[2], wgb.shape[2], wq_ref.shape[0]
    piece = xb.shape[1] // (2 * PAIRS)
    pair_n, rows_n, ffc = 2 * piece, NY * piece, 2 * ff
    half = PAIRS * pair_n
    row_p, row_m, partner = 2 * xp + c, 2 * xm + c, 2 * x + 1 - c
    ids = {n: i for i, n in enumerate(in_names())}
    copies = {}


    def define(name, src, dst, to_row, to_y):
        i = ids[name]
        copies[name] = to(src, dst, isend.at[i], irecv.at[i], to_row, to_y)

    def circle(name, ents, where, to_row, to_y):
        ref = xb.at[ents, where]
        define(name, ref, ref, to_row, to_y)

    def span(first, n):
        return pl.ds(pl.multiple_of(first * piece, piece), n * piece)

    blk = lambda i: pl.ds(2 * i, 2)
    ent = lambda i: pl.ds(i, 1)
    for k in range(SY):
        where = lambda j: span(2 * (NY * k + j), 2)
        for part, j in (("xp", row_p), ("xm", row_m)):
            if k == 0:
                circle(f"{part}0a", ent(row), where(y), j, y)
                circle(f"{part}0b", ent(partner), where(y), j, y)
            else:
                circle(f"{part}{k}", blk(x), where(y), j, y)
        circle(f"xpf{k}", ent(2 * xm), where(y), row_p, y)
        circle(f"xmf{k}", ent(2 * xp + 1), where(y), row_m, y)
        for tag, j in (("yp", yp), ("ym", ym)):
            for i, b in enumerate((xm, xp, x2)):
                circle(f"{tag}{i + 1}{k}", blk(b), where(y), row, j)
        circle(f"ypf1{k}", blk(xm), where(ym), row, yp)
        circle(f"ypf3{k}", ent(2 * x2), where(ym), row, yp)
        circle(f"ymf2{k}", blk(xp), where(yp), row, ym)
        circle(f"ymf3{k}", ent(2 * x2 + 1), where(yp), row, ym)
    for k in range(SX):
        where = pl.ds((2 * NY * SY + 2 * k) * piece, 2 * piece)
        circle(f"sp{k}", blk(x), where, row_p, y)
        circle(f"sm{k}", blk(x), where, row_m, y)
        circle(f"spf{k}", ent(2 * xm), where, row_p, y)
        circle(f"smf{k}", ent(2 * xp + 1), where, row_m, y)

    local = {}

    def bring(name, i, src_at, dst_at, n):
        there = xb.at[row, span(dst_at, n)]
        mine = pl.ds(pl.multiple_of(c * half + src_at * piece, piece), n * piece)
        theirs = pl.ds(pl.multiple_of((1 - c) * half + src_at * piece, piece), n * piece)
        local[name] = pltpu.make_async_copy(x_ref.at[mine], there, loc.at[i])
        define(name, x_ref.at[theirs], there, partner, y)

    for d in range(NY):
        j = lax.rem(y + d, NY)
        for k in range(SY):
            bring(f"d{d}{k}", d * SY + k, 2 * (NY * k + j), 2 * (NY * k + j), 2)
    for k in range(2 * SX):
        t, p = k // SX, k % SX
        bring(f"e{k}", NY * SY + k, 2 * (NY * SY + p) + t, 2 * NY * SY + k, 1)
    n_loc = NY * SY + 2 * SX
    for d in range(1, n_ent):
        define(f"g{d}0", g1_ref, g1b.at[row], lax.rem(row + d, n_ent), y)
        define(f"g{d}1", g2_ref, g2b.at[row], lax.rem(row + d, n_ent), y)
    define("wg", wg_ref, wgb.at[c], partner, y)
    define("wu", wu_ref, wub.at[c], partner, y)
    define("wd", wd_ref, wdx_ref, partner, y)
    weights = [
        pltpu.make_async_copy(g1_ref, g1b.at[row], loc.at[n_loc]),
        pltpu.make_async_copy(wg_ref, wgb.at[c], loc.at[n_loc + 1]),
        pltpu.make_async_copy(wu_ref, wub.at[c], loc.at[n_loc + 2]),
        pltpu.make_async_copy(g2_ref, g2b.at[row], loc.at[n_loc + 3]),
    ]
    start(local.values())
    start(weights)

    greet(
        [(lax.rem(row + d, n_ent), y) for d in range(1, n_ent)]
        + [(2 * x + h, lax.rem(y + d, NY)) for d in range(1, NY) for h in range(2)]
    )

    copies["d00"].start()
    local["d00"].wait()
    start([copies["xp0a"], copies["xm0a"]])
    own_rows = [f"d0{k}" for k in range(1, SY)]
    round_x = [n for n in local if n[0] == "e"]
    other_rows = [n for n in local if n[0] == "d" and n[1] != "0"]
    start([copies[n] for n in own_rows + round_x])
    start([copies[n] for n in other_rows + [f"g{d}{k}" for d in range(1, n_ent) for k in range(2)] + ["wg", "wu", "wd"]])

    def q(i, ref, to_row, to_y, src=None):
        return to(ref if src is None else src, ref, qsend.at[i], qrecv.at[i], to_row, to_y)

    def wq_at(b, off=0, n=qn):
        return wqa_ref.at[pl.ds(pl.multiple_of(b * qn + off, 16), n)]

    n_a = (qn // 2 + 15) // 16 * 16
    n_b = qn - n_a
    mine, b_m, b_p, b_2 = 2 * y + c, 2 * ym + c, 2 * yp + c, 2 * y2 + c
    src_a, src_b = wq_ref.at[pl.ds(0, n_a)], wq_ref.at[pl.ds(n_a, n_b)]
    qs = {
        QPA: q(QPA, wq_at(mine, 0, n_a), row, yp, src_a),
        QPB: q(QPB, wq_at(mine, n_a, n_b), row, yp, src_b),
        QMB: q(QMB, wq_at(mine, n_a, n_b), row, ym, src_b),
        QMA: q(QMA, wq_at(mine, 0, n_a), row, ym, src_a),
        QPF: q(QPF, wq_at(b_m, 0, n_a), row, yp),
        QMF: q(QMF, wq_at(b_p, n_a, n_b), row, ym),
        QD0: q(QD0, wq_at(mine), partner, y, wq_ref),
        QD1: q(QD1, wq_at(b_m), partner, y),
        QD2: q(QD2, wq_at(b_p), partner, y),
        QD3A: q(QD3A, wq_at(b_2, 0, n_a), partner, y),
        QD3B: q(QD3B, wq_at(b_2, n_a, n_b), partner, y),
    }
    start([qs[QPA], qs[QMB], qs[QD0]])
    got([copies["d00"]])
    start([copies["xp0b"], copies["xm0b"]])
    for n in own_rows:
        local[n].wait()
    got([copies[n] for n in own_rows])
    weights[0].wait()
    for first in range(0, qn, nt.shape[0]):
        n = min(nt.shape[0], qn - first)
        for a, b in ((wq_ref.at[pl.ds(first, n)], nt.at[pl.ds(0, n)]), (nt.at[pl.ds(0, n)], wq_at(mine, first, n))):
            cp = pltpu.make_async_copy(a, b, loc.at[n_loc])
            cp.start()
            cp.wait()

    def cols(i):
        return pl.ds(pl.multiple_of(i * ffc, 128), ffc)

    def at(i):
        return lax.rem(i + FIRST, TILES)

    def chunk_of(n):
        return lax.rem(n + FIRST // 2, CHUNKS)

    def rows(i, off=0, n=rows_n):
        return pl.ds(pl.multiple_of(at(i) * rows_n + off, 16), n)

    def ring(kind, j, src, dst, to_row, to_y):
        return to(src, dst, send.at[kind, j], recv.at[kind, j], to_row, to_y)

    def own(i):
        ref = aall.at[rows(i), cols(x)]
        return ring(AP, i, ref, ref, row_p, y), ring(AM, i, ref, ref, row_m, y)

    def onward(i):
        h = rows_n // 2
        up, down = aall.at[rows(i, 0, h), cols(xm)], aall.at[rows(i, h, h), cols(xp)]
        return ring(APF, i, up, up, row_p, y), ring(AMF, i, down, down, row_m, y)

    def act(tokens):
        for what, token in steps(tokens):
            group, k = token[:-1], int(token[-1])
            if what == "s" and token == FIRST_S:
                for n in round_x:
                    local[n].wait()
                got([copies[n] for n in round_x])
            if token == "q1":
                cps = [qs[QPB], qs[QMA]]
            elif token == "q2":
                got([qs[i] for i in (QPA, QMB, QPB, QMA)])
                cps = [qs[i] for i in (QPF, QMF, QD1, QD2)]
            elif group in ("a", "af"):
                cps = own(k) if group == "a" else onward(k)
            else:
                cps = []
                for part in GROUPS[group]:
                    cps += [copies[n] for n in ([f"{part}0a", f"{part}0b"] if token == "xp0" else [f"{part}{k}"])]
            if what == "w":
                got(cps)
            elif token != "xp0":
                start(cps)

    act(IN_PLAN[0])
    for cp in [local[n] for n in other_rows] + weights[1:]:
        cp.wait()
    got([copies[n] for n in other_rows])
    got([copies[n] for n in [f"g{d}{k}" for d in range(1, n_ent) for k in range(2)] + ["wg", "wu"]])

    base = {"s": y, "m": ym, "p": yp, "o": y2}

    def in_tile(s, _):
        for k in range(1, len(IN_TILES)):
            if IN_PLAN[k]:
                pl.when(s == k)(functools.partial(act, IN_PLAN[k]))
        first, p0, p1 = 0, 0, 0
        for k, name in enumerate(IN_TILES):
            i = int(name[1])
            if name[0] == "x":
                where = (2 * NY * SY + 2 * i, 2 * NY * SY + 2 * i, 2 * NY * SY + 2 * i + 1)
            else:
                j = base[name[0]]
                where = (2 * (NY * i + j), 2 * NY * i + j, 2 * NY * i + NY + j)
            first, p0, p1 = (jnp.where(s == k, a, b) for a, b in zip(where, (first, p0, p1)))

        def sixteen(g, _):
            r = pl.multiple_of(first * piece + g * 16, 16)
            d = pl.multiple_of(g * 16, 16)

            def store(e, v):
                nt[pl.ds(d, 16), e * width : (e + 1) * width] = v

            norm_rows(lambda e: xb[e, pl.ds(r, 16), :], g1b, store, n_ent, width)
            return 0

        lax.fori_loop(0, pair_n // 16, sixteen, 0)

        step = min(256, ff)
        for h in range(2):
            for col in range(0, ff, step):
                gate = jnp.dot(nt[...], wgb[h, :, col : col + step], preferred_element_type=F32)
                up = jnp.dot(nt[...], wub[h, :, col : col + step], preferred_element_type=F32)
                act_val = (gate * lax.logistic(gate) * up).astype(BF16)
                there = pl.ds(pl.multiple_of(x * ffc + h * ff + col, 128), step)
                for i, p in enumerate((p0, p1)):
                    aall[pl.ds(pl.multiple_of(p * piece, piece), piece), there] = act_val[i * piece : (i + 1) * piece]
        return 0

    lax.fori_loop(0, len(IN_TILES), in_tile, 0)
    act(IN_PLAN[-1])


    got([copies["wd"]])
    down = [
        pltpu.make_async_copy(wd_ref, wgb.at[c], loc.at[0]),
        pltpu.make_async_copy(wdx_ref, wgb.at[1 - c], loc.at[1]),
    ]
    start(down)
    for j in (row_p, row_m):
        pl.semaphore_signal(ready, inc=1, device_id={"row": j, "col": y}, device_id_type=MESH)
    for i in range(TILES):
        q_at, t = (i + FIRST) % TILES // 2, i % 2
        if q_at * NY < NY * SY:
            first = 2 * (NY * q_at + y) + t
        else:
            first = 2 * NY * SY + t * SX + y
        for h in range(2):
            xres[h, i] = xb[2 * x + h, span(first, 1), :]
    for n in ids:
        copies[n].wait_send()
    for cp in down:
        cp.wait()
    pl.semaphore_wait(ready, 2)


    def early(i):
        slot = lax.rem(i, SLOTS)
        return (
            ring(S1L, i, pbuf.at[slot, 0, y2], r1.at[i, 0], row, yp),
            ring(S1R, i, pbuf.at[slot, 1, y2], r1.at[i, 1], row, ym),
            ring(FR, i, pbuf.at[slot, 1, yp], rf.at[i, 1], row, yp),
            ring(GL, i, pbuf.at[slot, 0, ym], rf.at[i, 2], row, ym),
        )

    def late(i):
        slot = lax.rem(i, SLOTS)
        return (
            ring(FL, i, pbuf.at[slot, 0, yp], rf.at[i, 0], row, yp),
            ring(GR, i, pbuf.at[slot, 1, ym], rf.at[i, 3], row, ym),
        )

    def held(i, e, n=1):
        return wub.at[0, pl.ds(pl.multiple_of((i * n_ent + e) * piece, piece), n * piece)]

    def next_own(i):
        ref = held(i, 2 * x, 2)
        return ring(XP, i, ref, ref, row_p, y), ring(XM, i, ref, ref, row_m, y)

    def next_onward(i):
        up, down = held(i, 2 * xm), held(i, 2 * xp + 1)
        return ring(XPF, i, up, up, row_p, y), ring(XMF, i, down, down, row_m, y)

    def home(i, of_c, of_y):
        return resid_ref.at[of_c, lax.div(at(i), 2), of_y, lax.rem(i, 2)]

    def out(i):
        there = home(i, c, y)
        sends = []
        for h in range(2):
            src = held(i, 2 * x + h)
            sends.append(to(src, there, rsend.at[RP + h, i], rrecv.at[RP + c, i], 2 * x + h, yp))
            sends.append(to(src, there, rsend.at[RM + h, i], rrecv.at[RM + c, i], 2 * x + h, ym))
        sends.append(to(held(i, partner), there, rsend.at[RD, i], rrecv.at[RD, i], partner, y))
        return sends

    def out_own(i):
        return pltpu.make_async_copy(held(i, row), home(i, c, y), rloc.at[i])

    def out_arrived(i):
        return [to(held(i, row), home(i, 0, y), rsend.at[k, i], rrecv.at[k, i], row, yp) for k in range(4)]

    def relay(i):
        up, down = home(i, 0, ym), home(i, 1, yp)
        return (
            to(up, up, rsend.at[RPF, i], rrecv.at[RPF, i], row, yp),
            to(down, down, rsend.at[RMF, i], rrecv.at[RMF, i], row, ym),
        )

    def result(n, d, f):
        h = c if f == 0 else 1 - c
        to_y = lax.rem(y + d, NY)
        src = ob.at[n, 2 * to_y + h]
        first = (c * CHUNKS + chunk_of(n)) * NY + y
        dst = out_ref.at[:, pl.ds(pl.multiple_of(first * pair_n, 128), pair_n)]
        if d == 0 and f == 0:
            return pltpu.make_async_copy(src, dst, oloc.at[n])
        return to(src, dst, osend.at[n, 2 * d + f], orecv.at[n, 2 * d + f], 2 * x + h, to_y)

    def add_neighbour(i):
        got(early(i)[:2])
        slot = lax.rem(i, SLOTS)
        for r in range(0, piece, 16):
            s = pl.ds(r, 16)
            pbuf[slot, 0, yp, s, :] = pbuf[slot, 0, yp, s, :] + r1[i, 0, s, :]
            pbuf[slot, 1, ym, s, :] = pbuf[slot, 1, ym, s, :] + r1[i, 1, s, :]
        start(late(i))

    def final(i):
        got(early(i)[2:] + late(i))
        slot = lax.rem(i, SLOTS)
        for h in range(2):
            ref = held(i, 2 * x + h)
            for r in range(0, piece, 16):
                s = pl.ds(r, 16)
                total = pbuf[slot, h, y, s, :] + rf[i, h, s, :] + rf[i, 2 + h, s, :]
                ref[s, :] = (xres[h, i, s, :].astype(F32) + total).astype(BF16)

    def qkv(n):
        got(next_onward(2 * n) + next_onward(2 * n + 1))
        for t in range(2):

            def sixteen(g, _, t=t):
                r = pl.multiple_of(g * 16, 16)
                d = pl.multiple_of(t * piece + g * 16, 16)

                def store(e, v):
                    nt[pl.ds(d, 16), e * width : (e + 1) * width] = v

                norm_rows(lambda e: held(2 * n + t, e)[pl.ds(r, 16), :], g2b, store, n_ent, width)
                return 0

            lax.fori_loop(0, piece // 16, sixteen, 0)
        for b in range(0, 2 * NY, 2):
            part = None
            for e in range(n_ent):
                lhs, rhs = xb[e, b * qn : (b + 2) * qn, :], nt[:, e * width : (e + 1) * width]
                term = lax.dot_general(lhs, rhs, (((1,), (1,)), ((), ())), preferred_element_type=F32)
                part = term if part is None else part + term
            part = part.astype(BF16)
            for k in range(2):
                ob[n, b + k] = part[k * qn : (k + 1) * qn]
        for d in (2, 1, 3, 0):
            for f in range(2):
                result(n, d, f).start()

    def wq_load(e):
        src = wqa_ref.at[:, pl.ds(e * width, width)]
        return pltpu.make_async_copy(src, xb.at[e, pl.ds(0, 2 * NY * qn)], loc.at[e])

    step = min(256, width)

    def multiply(i):
        got(onward(i))

        @pl.when(i >= SLOTS)
        def _():
            for cp in early(i - SLOTS) + late(i - SLOTS):
                cp.wait_send()

        slot = lax.rem(i, SLOTS)
        for h in range(2):
            for col in range(0, width, step):
                part = jnp.dot(aall[rows(i), :], wgb[h, :, col : col + step], preferred_element_type=F32)
                for k in range(NY):
                    pbuf[slot, h, k, :, col : col + step] = part[k * piece : (k + 1) * piece]
        start(early(i))

    def light(tokens):
        for token in tokens:
            name, j = token[:-1], int(token[-1])
            if name == "a":
                start(own(j))
            elif name == "af":
                got(own(j))
                start(onward(j))
            elif name == "send":
                start(next_own(j))
            elif name == "pass":
                got(next_own(j))
                start(next_onward(j))
            elif name == "out":
                start(out(j) + [out_own(j)])
            elif name == "relay":
                got(out_arrived(j))
                start(relay(j))
            elif token == "q3":
                got([qs[QPF], qs[QMF]])
                start([qs[QD3A], qs[QD3B]])
            elif token == "q4":
                got([qs[k] for k in (QD0, QD1, QD2, QD3A, QD3B)])
                start([wq_load(e) for e in range(n_ent)])
            elif token == "q5":
                for e in range(n_ent):
                    wq_load(e).wait()

    bodies = {"mm": multiply, "add": add_neighbour, "fin": final, "qkv": qkv}

    def out_step(s, _):
        for k, tokens in enumerate(LIGHT):
            if tokens:
                pl.when(s == k)(functools.partial(light, tokens))
        kind, j = KINDS.index(HEAVY[0][0]), HEAVY[0][1]
        for k, (name, i) in enumerate(HEAVY[1:]):
            kind = jnp.where(s == k + 1, KINDS.index(name), kind)
            j = jnp.where(s == k + 1, i, j)
        for k, name in enumerate(KINDS):
            pl.when(kind == k)(functools.partial(bodies[name], j))
        return 0

    lax.fori_loop(0, len(HEAVY), out_step, 0)

    def settle(i, _):
        for cp in own(i) + onward(i) + next_own(i) + next_onward(i):
            cp.wait_send()
        for cp in out(i) + list(relay(i)):
            cp.wait_send()
        got([out(i)[-1]] + list(relay(i)))
        out_own(i).wait()

        @pl.when(i >= TILES - SLOTS)
        def _():
            for cp in early(i) + late(i):
                cp.wait_send()

        return 0

    lax.fori_loop(0, TILES, settle, 0)

    def settle_out(n, _):
        for d in range(NY):
            for f in range(2):
                result(n, d, f).wait()
        return 0

    lax.fori_loop(0, CHUNKS, settle_out, 0)
    for i in qs:
        qs[i].wait_send()


def hand_over(a_ref, b_ref, a_out, b_out, a_buf, b_buf, a_in_sem, a_out_sem, b_sem):
    n = a_in_sem.shape[0]
    rows = a_ref.shape[0] // n
    part = lambda ref, i: ref.at[pl.ds(i * rows, rows)]
    ins = [pltpu.make_async_copy(part(a_ref, i), part(a_buf, i), a_in_sem.at[i]) for i in range(n)]
    outs = [pltpu.make_async_copy(part(a_buf, i), part(a_out, i), a_out_sem.at[i]) for i in range(n)]
    b_in = pltpu.make_async_copy(b_ref, b_buf, b_sem.at[0])
    b_back = pltpu.make_async_copy(b_buf, b_out, b_sem.at[1])
    start(ins + [b_in])
    for i in range(n):
        ins[i].wait()
        outs[i].start()
    b_in.wait()
    b_back.start()
    for cp in outs + [b_back]:
        cp.wait()


def solution(mesh):
    assert mesh.shape["row"] == 2 * NX and mesh.shape["col"] == NY
    tok_spec, gain_spec = P("data", "row"), P("row")
    wide_spec, down_spec, qkv_spec = P(None, ("col", "row")), P("col", "row"), P("data", ("col", "row"))

    def per_device(residual, gain_mlp, gain_attn, w_gate, w_up, w_down, w_qkv):
        tokens, width = residual.shape
        hidden, ff = w_gate.shape
        qn = w_qkv.shape[1]
        half = tokens // 2
        piece = half // PAIRS // 2
        n_ent = 2 * NX
        n_in = len(in_names())
        resid, qkv_t, _, _ = pl.pallas_call(
            kernel,
            name="mlp_qkv",
            out_shape=[
                jax.ShapeDtypeStruct((2, CHUNKS, NY, 2, piece, width), BF16),
                jax.ShapeDtypeStruct((qn, tokens), BF16),
                jax.ShapeDtypeStruct((n_ent * ff, width), BF16),
                jax.ShapeDtypeStruct((2 * NY * qn, hidden), BF16),
            ],
            in_specs=[ANY] * 7,
            out_specs=[ANY] * 4,
            scratch_shapes=[
                pltpu.VMEM((n_ent, half, width), BF16),
                pltpu.VMEM((2, hidden, ff), BF16),
                pltpu.VMEM((2, hidden, ff), BF16),
                pltpu.VMEM((half, n_ent * ff), BF16),
                pltpu.VMEM((SLOTS, 2, NY, piece, width), F32),
                pltpu.VMEM((TILES, 2, piece, width), F32),
                pltpu.VMEM((TILES, 4, piece, width), F32),
                pltpu.VMEM((2, TILES, piece, width), BF16),
                pltpu.VMEM((2 * piece, hidden), BF16),
                pltpu.VMEM((n_ent, 1, width), F32),
                pltpu.VMEM((n_ent, 1, width), F32),
                pltpu.VMEM((CHUNKS, 2 * NY, qn, 2 * piece), BF16),
                DMA((n_in,)),
                DMA((n_in,)),
                DMA((14, TILES)),
                DMA((14, TILES)),
                DMA((11,)),
                DMA((11,)),
                DMA((7, TILES)),
                DMA((7, TILES)),
                DMA((CHUNKS, 2 * NY)),
                DMA((CHUNKS, 2 * NY)),
                DMA((NY * SY + 2 * SX + 4,)),
                DMA((TILES,)),
                DMA((CHUNKS,)),
                pltpu.SemaphoreType.REGULAR,
            ],
            compiler_params=pltpu.CompilerParams(collective_id=1, has_side_effects=True, vmem_limit_bytes=LIMIT),
        )(residual, gain_mlp[None], gain_attn[None], w_gate, w_up, w_down, w_qkv.T)
        parts = 2
        resid, qkv_t = pl.pallas_call(
            hand_over,
            name="hand_over",
            out_shape=[jax.ShapeDtypeStruct((tokens, width), BF16), jax.ShapeDtypeStruct((qn, tokens), BF16)],
            in_specs=[ANY] * 2,
            out_specs=[ANY] * 2,
            scratch_shapes=[
                pltpu.VMEM((tokens, width), BF16),
                pltpu.VMEM((qn, tokens), BF16),
                DMA((parts,)),
                DMA((parts,)),
                DMA((2,)),
            ],
        )(resid.reshape(tokens, width), qkv_t)
        return resid, qkv_t.T

    return jax.shard_map(
        per_device,
        mesh=mesh,
        in_specs=(tok_spec, gain_spec, gain_spec, wide_spec, wide_spec, down_spec, wide_spec),
        out_specs=(tok_spec, qkv_spec),
        check_vma=False,
    )
```

```python
import functools

import jax
import jax.numpy as jnp
from jax import lax
from jax.experimental import pallas as pl
from jax.experimental.pallas import tpu as pltpu
from jax.sharding import PartitionSpec as P

NORM_EPS = 1e-6
MESH = pl.DeviceIdType.MESH
BF16 = jnp.bfloat16
F32 = jnp.float32
ANY = pl.BlockSpec(memory_space=pl.ANY)
VMEM = pl.BlockSpec(memory_space=pltpu.VMEM)
DMA = pltpu.SemaphoreType.DMA
LIMIT = 64 * 1024 * 1024 - 128 * 1024

NX, NY = 4, 4
PAIRS = 16
SY = 3
SX = PAIRS - NY * SY
TILES = PAIRS // 2
CHUNKS = TILES // 2
FIRST = NY * SY // 2
SLOTS = 4


def place():
    row, y = lax.axis_index("row"), lax.axis_index("col")
    return lax.div(row, 2), lax.rem(row, 2), row, y


def around(i, n):
    return lax.rem(i + 1, n), lax.rem(i + n - 1, n), lax.rem(i + 2, n)


def greet(peers):
    barrier = pltpu.get_barrier_semaphore()
    for row, y in peers:
        pl.semaphore_signal(barrier, inc=1, device_id={"row": row, "col": y}, device_id_type=MESH)
    pl.semaphore_wait(barrier, len(peers))


def to(src, dst, send, recv, row, y):
    return pltpu.make_async_remote_copy(src, dst, send, recv, device_id={"row": row, "col": y}, device_id_type=MESH)


def start(copies):
    for cp in copies:
        cp.start()


def got(copies):
    for cp in copies:
        cp.wait_recv()


def norm_rows(load, gains, store, n_ent, width):
    acc = None
    for e in range(n_ent):
        v = load(e).astype(F32)
        acc = v * v if acc is None else acc + v * v
    scale = lax.rsqrt(jnp.sum(acc, axis=1, keepdims=True) / (n_ent * width) + NORM_EPS)
    for e in range(n_ent):
        store(e, (load(e).astype(F32) * scale * gains[e]).astype(BF16))


def steps(tokens):
    out, what = [], None
    for token in tokens:
        if token in ("s", "w"):
            what = token
        else:
            out.append((what, token))
    return out


GROUPS = {
    "xp": ("xp", "xm"),
    "xf": ("xpf", "xmf"),
    "ya": ("yp1", "yp2", "ym1", "ym2"),
    "yb": ("yp3", "ym3"),
    "yf": ("ypf1", "ypf3", "ymf2", "ymf3"),
    "s": ("sp", "sm"),
    "sf": ("spf", "smf"),
}
COUNTS = {"xp": SY, "xf": SY, "ya": SY, "yb": SY, "yf": SY, "s": SX, "sf": SX}

IN_TILES = ("p0", "m0", "s1", "s0", "o0", "x1", "s2", "x2", "x0", "x3", "o1", "p2", "m1", "p1", "m2", "o2")
IN_PLAN = (
    ("s", "xp0", "s1", "s2", "w", "xp0", "s", "xf0", "xp1", "ya0", "s3", "w", "xf0", "s", "yb0", "w", "xp1", "s", "xf1", "w", "s1", "s", "sf1", "xp2", "w", "ya0", "yb0", "s", "yf0", "w", "s3", "s", "sf3"),
    ("s", "ya1"),
    ("s", "s0", "w", "s2", "s", "sf2", "w", "xf1"),
    (),
    ("w", "yf0"),
    ("w", "xp2", "s", "xf2", "a3", "ya2", "w", "sf1"),
    ("w", "xf2"),
    ("w", "s0", "s", "sf0", "yb1", "a2", "yb2", "w", "ya1", "yb1", "s", "yf1", "w", "sf2"),
    ("w", "sf0"),
    ("w", "a3", "s", "af3", "w", "sf3"),
    ("s", "a1", "q1", "a0", "w", "ya2", "yb2", "s", "yf2", "w", "yf1"),
    (),
    (),
    ("w", "a1", "s", "af1", "w", "a2", "s", "af2"),
    ("s", "q2"),
    ("w", "yf2"),
    ("w", "a0", "s", "af0"),
)

HEAVY = (
    ("mm", 1),
    ("mm", 3),
    ("add", 1),
    ("mm", 0),
    ("add", 3),
    ("mm", 2),
    ("fin", 1),
    ("add", 0),
    ("add", 2),
    ("fin", 3),
    ("fin", 0),
    ("mm", 5),
    ("add", 5),
    ("fin", 2),
    ("fin", 5),
    ("mm", 4),
    ("add", 4),
    ("mm", 6),
    ("fin", 4),
    ("add", 6),
    ("mm", 7),
    ("fin", 6),
    ("add", 7),
    ("fin", 7),
    ("qkv", 2),
    ("qkv", 1),
    ("qkv", 0),
    ("qkv", 3),
)
LIGHT = (
    ("a5",),
    (),
    (),
    ("a4",),
    (),
    (),
    ("q3", "af5"),
    ("a6",),
    (),
    ("out1",),
    (),
    ("af4", "out0"),
    (),
    ("out3", "af6"),
    (),
    ("a7", "out5", "relay0"),
    ("relay1",),
    ("send5",),
    (),
    ("af7", "send4", "out2", "send2", "out4", "send3"),
    ("q4", "relay2", "send1"),
    ("pass5", "pass4"),
    ("send0", "out6", "pass2"),
    ("send6", "pass3", "relay3", "relay4", "relay6"),
    ("relay5", "send7", "pass0", "out7", "pass1", "q5"),
    ("pass6",),
    ("relay7", "pass7"),
    (),
)
KINDS = ("mm", "add", "fin", "qkv")
FIRST_S = next(n for n in IN_PLAN[0] if n[0] == "s" and n[1:].isdigit())


def in_names():
    names = []
    for group, parts in GROUPS.items():
        for k in range(COUNTS[group]):
            for part in parts:
                names += [f"{part}{k}a", f"{part}{k}b"] if group == "xp" and k == 0 else [f"{part}{k}"]
    names += [f"d{d}{k}" for d in range(NY) for k in range(SY)] + [f"e{s}" for s in range(2 * SX)]
    names += [f"g{d}{k}" for d in range(1, 2 * NX) for k in range(2)]
    return names + ["wg", "wu", "wd"]


AP, AM, APF, AMF, S1L, S1R, FL, FR, GL, GR, XP, XM, XPF, XMF = range(14)
QPA, QPB, QMB, QMA, QPF, QMF, QD0, QD1, QD2, QD3A, QD3B = range(11)
RP, RM, RPF, RMF, RD = 0, 2, 4, 5, 6


def kernel(
    x_ref, g1_ref, g2_ref, wg_ref, wu_ref, wd_ref, wq_ref, resid_ref, out_ref, wdx_ref, wqa_ref,
    xb, wgb, wub, aall, pbuf, r1, rf, xres, nt, g1b, g2b, ob,
    isend, irecv, send, recv, qsend, qrecv, rsend, rrecv, osend, orecv, loc, rloc, oloc, ready,
):
    x, c, row, y = place()
    xp, xm, x2 = around(x, NX)
    yp, ym, y2 = around(y, NY)
    n_ent = 2 * NX
    width, ff, qn = xb.shape[2], wgb.shape[2], wq_ref.shape[0]
    piece = xb.shape[1] // (2 * PAIRS)
    pair_n, rows_n, ffc = 2 * piece, NY * piece, 2 * ff
    half = PAIRS * pair_n
    row_p, row_m, partner = 2 * xp + c, 2 * xm + c, 2 * x + 1 - c
    ids = {n: i for i, n in enumerate(in_names())}
    copies = {}


    def define(name, src, dst, to_row, to_y):
        i = ids[name]
        copies[name] = to(src, dst, isend.at[i], irecv.at[i], to_row, to_y)

    def circle(name, ents, where, to_row, to_y):
        ref = xb.at[ents, where]
        define(name, ref, ref, to_row, to_y)

    def span(first, n):
        return pl.ds(pl.multiple_of(first * piece, piece), n * piece)

    blk = lambda i: pl.ds(2 * i, 2)
    ent = lambda i: pl.ds(i, 1)
    for k in range(SY):
        where = lambda j: span(2 * (NY * k + j), 2)
        for part, j in (("xp", row_p), ("xm", row_m)):
            if k == 0:
                circle(f"{part}0a", ent(row), where(y), j, y)
                circle(f"{part}0b", ent(partner), where(y), j, y)
            else:
                circle(f"{part}{k}", blk(x), where(y), j, y)
        circle(f"xpf{k}", ent(2 * xm), where(y), row_p, y)
        circle(f"xmf{k}", ent(2 * xp + 1), where(y), row_m, y)
        for tag, j in (("yp", yp), ("ym", ym)):
            for i, b in enumerate((xm, xp, x2)):
                circle(f"{tag}{i + 1}{k}", blk(b), where(y), row, j)
        circle(f"ypf1{k}", blk(xm), where(ym), row, yp)
        circle(f"ypf3{k}", ent(2 * x2), where(ym), row, yp)
        circle(f"ymf2{k}", blk(xp), where(yp), row, ym)
        circle(f"ymf3{k}", ent(2 * x2 + 1), where(yp), row, ym)
    for k in range(SX):
        where = pl.ds((2 * NY * SY + 2 * k) * piece, 2 * piece)
        circle(f"sp{k}", blk(x), where, row_p, y)
        circle(f"sm{k}", blk(x), where, row_m, y)
        circle(f"spf{k}", ent(2 * xm), where, row_p, y)
        circle(f"smf{k}", ent(2 * xp + 1), where, row_m, y)

    local = {}

    def bring(name, i, src_at, dst_at, n):
        there = xb.at[row, span(dst_at, n)]
        mine = pl.ds(pl.multiple_of(c * half + src_at * piece, piece), n * piece)
        theirs = pl.ds(pl.multiple_of((1 - c) * half + src_at * piece, piece), n * piece)
        local[name] = pltpu.make_async_copy(x_ref.at[mine], there, loc.at[i])
        define(name, x_ref.at[theirs], there, partner, y)

    for d in range(NY):
        j = lax.rem(y + d, NY)
        for k in range(SY):
            bring(f"d{d}{k}", d * SY + k, 2 * (NY * k + j), 2 * (NY * k + j), 2)
    for k in range(2 * SX):
        t, p = k // SX, k % SX
        bring(f"e{k}", NY * SY + k, 2 * (NY * SY + p) + t, 2 * NY * SY + k, 1)
    n_loc = NY * SY + 2 * SX
    for d in range(1, n_ent):
        define(f"g{d}0", g1_ref, g1b.at[row], lax.rem(row + d, n_ent), y)
        define(f"g{d}1", g2_ref, g2b.at[row], lax.rem(row + d, n_ent), y)
    define("wg", wg_ref, wgb.at[c], partner, y)
    define("wu", wu_ref, wub.at[c], partner, y)
    define("wd", wd_ref, wdx_ref, partner, y)
    weights = [
        pltpu.make_async_copy(g1_ref, g1b.at[row], loc.at[n_loc]),
        pltpu.make_async_copy(wg_ref, wgb.at[c], loc.at[n_loc + 1]),
        pltpu.make_async_copy(wu_ref, wub.at[c], loc.at[n_loc + 2]),
        pltpu.make_async_copy(g2_ref, g2b.at[row], loc.at[n_loc + 3]),
    ]
    start(local.values())
    start(weights)

    greet(
        [(lax.rem(row + d, n_ent), y) for d in range(1, n_ent)]
        + [(2 * x + h, lax.rem(y + d, NY)) for d in range(1, NY) for h in range(2)]
    )

    copies["d00"].start()
    local["d00"].wait()
    start([copies["xp0a"], copies["xm0a"]])
    own_rows = [f"d0{k}" for k in range(1, SY)]
    round_x = [n for n in local if n[0] == "e"]
    other_rows = [n for n in local if n[0] == "d" and n[1] != "0"]
    start([copies[n] for n in own_rows + round_x])
    start([copies[n] for n in other_rows + [f"g{d}{k}" for d in range(1, n_ent) for k in range(2)] + ["wg", "wu", "wd"]])

    def q(i, ref, to_row, to_y, src=None):
        return to(ref if src is None else src, ref, qsend.at[i], qrecv.at[i], to_row, to_y)

    def wq_at(b, off=0, n=qn):
        return wqa_ref.at[pl.ds(pl.multiple_of(b * qn + off, 16), n)]

    n_a = (qn // 2 + 15) // 16 * 16
    n_b = qn - n_a
    mine, b_m, b_p, b_2 = 2 * y + c, 2 * ym + c, 2 * yp + c, 2 * y2 + c
    src_a, src_b = wq_ref.at[pl.ds(0, n_a)], wq_ref.at[pl.ds(n_a, n_b)]
    qs = {
        QPA: q(QPA, wq_at(mine, 0, n_a), row, yp, src_a),
        QPB: q(QPB, wq_at(mine, n_a, n_b), row, yp, src_b),
        QMB: q(QMB, wq_at(mine, n_a, n_b), row, ym, src_b),
        QMA: q(QMA, wq_at(mine, 0, n_a), row, ym, src_a),
        QPF: q(QPF, wq_at(b_m, 0, n_a), row, yp),
        QMF: q(QMF, wq_at(b_p, n_a, n_b), row, ym),
        QD0: q(QD0, wq_at(mine), partner, y, wq_ref),
        QD1: q(QD1, wq_at(b_m), partner, y),
        QD2: q(QD2, wq_at(b_p), partner, y),
        QD3A: q(QD3A, wq_at(b_2, 0, n_a), partner, y),
        QD3B: q(QD3B, wq_at(b_2, n_a, n_b), partner, y),
    }
    start([qs[QPA], qs[QMB], qs[QD0]])
    got([copies["d00"]])
    start([copies["xp0b"], copies["xm0b"]])
    for n in own_rows:
        local[n].wait()
    got([copies[n] for n in own_rows])
    weights[0].wait()
    for first in range(0, qn, nt.shape[0]):
        n = min(nt.shape[0], qn - first)
        for a, b in ((wq_ref.at[pl.ds(first, n)], nt.at[pl.ds(0, n)]), (nt.at[pl.ds(0, n)], wq_at(mine, first, n))):
            cp = pltpu.make_async_copy(a, b, loc.at[n_loc])
            cp.start()
            cp.wait()

    def cols(i):
        return pl.ds(pl.multiple_of(i * ffc, 128), ffc)

    def at(i):
        return lax.rem(i + FIRST, TILES)

    def chunk_of(n):
        return lax.rem(n + FIRST // 2, CHUNKS)

    def rows(i, off=0, n=rows_n):
        return pl.ds(pl.multiple_of(at(i) * rows_n + off, 16), n)

    def ring(kind, j, src, dst, to_row, to_y):
        return to(src, dst, send.at[kind, j], recv.at[kind, j], to_row, to_y)

    def own(i):
        ref = aall.at[rows(i), cols(x)]
        return ring(AP, i, ref, ref, row_p, y), ring(AM, i, ref, ref, row_m, y)

    def onward(i):
        h = rows_n // 2
        up, down = aall.at[rows(i, 0, h), cols(xm)], aall.at[rows(i, h, h), cols(xp)]
        return ring(APF, i, up, up, row_p, y), ring(AMF, i, down, down, row_m, y)

    def act(tokens):
        for what, token in steps(tokens):
            group, k = token[:-1], int(token[-1])
            if what == "s" and token == FIRST_S:
                for n in round_x:
                    local[n].wait()
                got([copies[n] for n in round_x])
            if token == "q1":
                cps = [qs[QPB], qs[QMA]]
            elif token == "q2":
                got([qs[i] for i in (QPA, QMB, QPB, QMA)])
                cps = [qs[i] for i in (QPF, QMF, QD1, QD2)]
            elif group in ("a", "af"):
                cps = own(k) if group == "a" else onward(k)
            else:
                cps = []
                for part in GROUPS[group]:
                    cps += [copies[n] for n in ([f"{part}0a", f"{part}0b"] if token == "xp0" else [f"{part}{k}"])]
            if what == "w":
                got(cps)
            elif token != "xp0":
                start(cps)

    act(IN_PLAN[0])
    for cp in [local[n] for n in other_rows] + weights[1:]:
        cp.wait()
    got([copies[n] for n in other_rows])
    got([copies[n] for n in [f"g{d}{k}" for d in range(1, n_ent) for k in range(2)] + ["wg", "wu"]])

    base = {"s": y, "m": ym, "p": yp, "o": y2}

    def in_tile(s, _):
        for k in range(1, len(IN_TILES)):
            if IN_PLAN[k]:
                pl.when(s == k)(functools.partial(act, IN_PLAN[k]))
        first, p0, p1 = 0, 0, 0
        for k, name in enumerate(IN_TILES):
            i = int(name[1])
            if name[0] == "x":
                where = (2 * NY * SY + 2 * i, 2 * NY * SY + 2 * i, 2 * NY * SY + 2 * i + 1)
            else:
                j = base[name[0]]
                where = (2 * (NY * i + j), 2 * NY * i + j, 2 * NY * i + NY + j)
            first, p0, p1 = (jnp.where(s == k, a, b) for a, b in zip(where, (first, p0, p1)))

        def sixteen(g, _):
            r = pl.multiple_of(first * piece + g * 16, 16)
            d = pl.multiple_of(g * 16, 16)

            def store(e, v):
                nt[pl.ds(d, 16), e * width : (e + 1) * width] = v

            norm_rows(lambda e: xb[e, pl.ds(r, 16), :], g1b, store, n_ent, width)
            return 0

        lax.fori_loop(0, pair_n // 16, sixteen, 0)

        step = min(256, ff)
        for h in range(2):
            for col in range(0, ff, step):
                gate = jnp.dot(nt[...], wgb[h, :, col : col + step], preferred_element_type=F32)
                up = jnp.dot(nt[...], wub[h, :, col : col + step], preferred_element_type=F32)
                act_val = (gate * lax.logistic(gate) * up).astype(BF16)
                there = pl.ds(pl.multiple_of(x * ffc + h * ff + col, 128), step)
                for i, p in enumerate((p0, p1)):
                    aall[pl.ds(pl.multiple_of(p * piece, piece), piece), there] = act_val[i * piece : (i + 1) * piece]
        return 0

    lax.fori_loop(0, len(IN_TILES), in_tile, 0)
    act(IN_PLAN[-1])


    got([copies["wd"]])
    down = [
        pltpu.make_async_copy(wd_ref, wgb.at[c], loc.at[0]),
        pltpu.make_async_copy(wdx_ref, wgb.at[1 - c], loc.at[1]),
    ]
    start(down)
    for j in (row_p, row_m):
        pl.semaphore_signal(ready, inc=1, device_id={"row": j, "col": y}, device_id_type=MESH)
    for i in range(TILES):
        q_at, t = (i + FIRST) % TILES // 2, i % 2
        if q_at * NY < NY * SY:
            first = 2 * (NY * q_at + y) + t
        else:
            first = 2 * NY * SY + t * SX + y
        for h in range(2):
            xres[h, i] = xb[2 * x + h, span(first, 1), :]
    for n in ids:
        copies[n].wait_send()
    for cp in down:
        cp.wait()
    pl.semaphore_wait(ready, 2)


    def early(i):
        slot = lax.rem(i, SLOTS)
        return (
            ring(S1L, i, pbuf.at[slot, 0, y2], r1.at[i, 0], row, yp),
            ring(S1R, i, pbuf.at[slot, 1, y2], r1.at[i, 1], row, ym),
            ring(FR, i, pbuf.at[slot, 1, yp], rf.at[i, 1], row, yp),
            ring(GL, i, pbuf.at[slot, 0, ym], rf.at[i, 2], row, ym),
        )

    def late(i):
        slot = lax.rem(i, SLOTS)
        return (
            ring(FL, i, pbuf.at[slot, 0, yp], rf.at[i, 0], row, yp),
            ring(GR, i, pbuf.at[slot, 1, ym], rf.at[i, 3], row, ym),
        )

    def held(i, e, n=1):
        return wub.at[0, pl.ds(pl.multiple_of((i * n_ent + e) * piece, piece), n * piece)]

    def next_own(i):
        ref = held(i, 2 * x, 2)
        return ring(XP, i, ref, ref, row_p, y), ring(XM, i, ref, ref, row_m, y)

    def next_onward(i):
        up, down = held(i, 2 * xm), held(i, 2 * xp + 1)
        return ring(XPF, i, up, up, row_p, y), ring(XMF, i, down, down, row_m, y)

    def home(i, of_c, of_y):
        return resid_ref.at[of_c, lax.div(at(i), 2), of_y, lax.rem(i, 2)]

    def out(i):
        there = home(i, c, y)
        sends = []
        for h in range(2):
            src = held(i, 2 * x + h)
            sends.append(to(src, there, rsend.at[RP + h, i], rrecv.at[RP + c, i], 2 * x + h, yp))
            sends.append(to(src, there, rsend.at[RM + h, i], rrecv.at[RM + c, i], 2 * x + h, ym))
        sends.append(to(held(i, partner), there, rsend.at[RD, i], rrecv.at[RD, i], partner, y))
        return sends

    def out_own(i):
        return pltpu.make_async_copy(held(i, row), home(i, c, y), rloc.at[i])

    def out_arrived(i):
        return [to(held(i, row), home(i, 0, y), rsend.at[k, i], rrecv.at[k, i], row, yp) for k in range(4)]

    def relay(i):
        up, down = home(i, 0, ym), home(i, 1, yp)
        return (
            to(up, up, rsend.at[RPF, i], rrecv.at[RPF, i], row, yp),
            to(down, down, rsend.at[RMF, i], rrecv.at[RMF, i], row, ym),
        )

    def result(n, d, f):
        h = c if f == 0 else 1 - c
        to_y = lax.rem(y + d, NY)
        src = ob.at[n, 2 * to_y + h]
        first = (c * CHUNKS + chunk_of(n)) * NY + y
        dst = out_ref.at[:, pl.ds(pl.multiple_of(first * pair_n, 128), pair_n)]
        if d == 0 and f == 0:
            return pltpu.make_async_copy(src, dst, oloc.at[n])
        return to(src, dst, osend.at[n, 2 * d + f], orecv.at[n, 2 * d + f], 2 * x + h, to_y)

    def add_neighbour(i):
        got(early(i)[:2])
        slot = lax.rem(i, SLOTS)
        for r in range(0, piece, 16):
            s = pl.ds(r, 16)
            pbuf[slot, 0, yp, s, :] = pbuf[slot, 0, yp, s, :] + r1[i, 0, s, :]
            pbuf[slot, 1, ym, s, :] = pbuf[slot, 1, ym, s, :] + r1[i, 1, s, :]
        start(late(i))

    def final(i):
        got(early(i)[2:] + late(i))
        slot = lax.rem(i, SLOTS)
        for h in range(2):
            ref = held(i, 2 * x + h)
            for r in range(0, piece, 16):
                s = pl.ds(r, 16)
                total = pbuf[slot, h, y, s, :] + rf[i, h, s, :] + rf[i, 2 + h, s, :]
                ref[s, :] = (xres[h, i, s, :].astype(F32) + total).astype(BF16)

    def qkv(n):
        got(next_onward(2 * n) + next_onward(2 * n + 1))
        for t in range(2):

            def sixteen(g, _, t=t):
                r = pl.multiple_of(g * 16, 16)
                d = pl.multiple_of(t * piece + g * 16, 16)

                def store(e, v):
                    nt[pl.ds(d, 16), e * width : (e + 1) * width] = v

                norm_rows(lambda e: held(2 * n + t, e)[pl.ds(r, 16), :], g2b, store, n_ent, width)
                return 0

            lax.fori_loop(0, piece // 16, sixteen, 0)
        for b in range(0, 2 * NY, 2):
            part = None
            for e in range(n_ent):
                lhs, rhs = xb[e, b * qn : (b + 2) * qn, :], nt[:, e * width : (e + 1) * width]
                term = lax.dot_general(lhs, rhs, (((1,), (1,)), ((), ())), preferred_element_type=F32)
                part = term if part is None else part + term
            part = part.astype(BF16)
            for k in range(2):
                ob[n, b + k] = part[k * qn : (k + 1) * qn]
        for d in (2, 1, 3, 0):
            for f in range(2):
                result(n, d, f).start()

    def wq_load(e):
        src = wqa_ref.at[:, pl.ds(e * width, width)]
        return pltpu.make_async_copy(src, xb.at[e, pl.ds(0, 2 * NY * qn)], loc.at[e])

    step = min(256, width)

    def multiply(i):
        got(onward(i))

        @pl.when(i >= SLOTS)
        def _():
            for cp in early(i - SLOTS) + late(i - SLOTS):
                cp.wait_send()

        slot = lax.rem(i, SLOTS)
        for h in range(2):
            for col in range(0, width, step):
                part = jnp.dot(aall[rows(i), :], wgb[h, :, col : col + step], preferred_element_type=F32)
                for k in range(NY):
                    pbuf[slot, h, k, :, col : col + step] = part[k * piece : (k + 1) * piece]
        start(early(i))

    def light(tokens):
        for token in tokens:
            name, j = token[:-1], int(token[-1])
            if name == "a":
                start(own(j))
            elif name == "af":
                got(own(j))
                start(onward(j))
            elif name == "send":
                start(next_own(j))
            elif name == "pass":
                got(next_own(j))
                start(next_onward(j))
            elif name == "out":
                start(out(j) + [out_own(j)])
            elif name == "relay":
                got(out_arrived(j))
                start(relay(j))
            elif token == "q3":
                got([qs[QPF], qs[QMF]])
                start([qs[QD3A], qs[QD3B]])
            elif token == "q4":
                got([qs[k] for k in (QD0, QD1, QD2, QD3A, QD3B)])
                start([wq_load(e) for e in range(n_ent)])
            elif token == "q5":
                for e in range(n_ent):
                    wq_load(e).wait()

    bodies = {"mm": multiply, "add": add_neighbour, "fin": final, "qkv": qkv}

    def out_step(s, _):
        for k, tokens in enumerate(LIGHT):
            if tokens:
                pl.when(s == k)(functools.partial(light, tokens))
        kind, j = KINDS.index(HEAVY[0][0]), HEAVY[0][1]
        for k, (name, i) in enumerate(HEAVY[1:]):
            kind = jnp.where(s == k + 1, KINDS.index(name), kind)
            j = jnp.where(s == k + 1, i, j)
        for k, name in enumerate(KINDS):
            pl.when(kind == k)(functools.partial(bodies[name], j))
        return 0

    lax.fori_loop(0, len(HEAVY), out_step, 0)

    def settle(i, _):
        for cp in own(i) + onward(i) + next_own(i) + next_onward(i):
            cp.wait_send()
        for cp in out(i) + list(relay(i)):
            cp.wait_send()
        got([out(i)[-1]] + list(relay(i)))
        out_own(i).wait()

        @pl.when(i >= TILES - SLOTS)
        def _():
            for cp in early(i) + late(i):
                cp.wait_send()

        return 0

    lax.fori_loop(0, TILES, settle, 0)

    def settle_out(n, _):
        for d in range(NY):
            for f in range(2):
                result(n, d, f).wait()
        return 0

    lax.fori_loop(0, CHUNKS, settle_out, 0)
    for i in qs:
        qs[i].wait_send()


def hand_over(a_ref, b_ref, a_out, b_out, a_buf, b_buf, a_in_sem, a_out_sem, b_sem):
    n = a_in_sem.shape[0]
    rows = a_ref.shape[0] // n
    part = lambda ref, i: ref.at[pl.ds(i * rows, rows)]
    ins = [pltpu.make_async_copy(part(a_ref, i), part(a_buf, i), a_in_sem.at[i]) for i in range(n)]
    outs = [pltpu.make_async_copy(part(a_buf, i), part(a_out, i), a_out_sem.at[i]) for i in range(n)]
    b_in = pltpu.make_async_copy(b_ref, b_buf, b_sem.at[0])
    b_back = pltpu.make_async_copy(b_buf, b_out, b_sem.at[1])
    start(ins + [b_in])
    for i in range(n):
        ins[i].wait()
        outs[i].start()
    b_in.wait()
    b_back.start()
    for cp in outs + [b_back]:
        cp.wait()


def solution(mesh):
    assert mesh.shape["row"] == 2 * NX and mesh.shape["col"] == NY
    tok_spec, gain_spec = P("data", "row"), P("row")
    wide_spec, down_spec, qkv_spec = P(None, ("col", "row")), P("col", "row"), P("data", ("col", "row"))

    def per_device(residual, gain_mlp, gain_attn, w_gate, w_up, w_down, w_qkv):
        tokens, width = residual.shape
        hidden, ff = w_gate.shape
        qn = w_qkv.shape[1]
        half = tokens // 2
        piece = half // PAIRS // 2
        n_ent = 2 * NX
        n_in = len(in_names())
        resid, qkv_t, _, _ = pl.pallas_call(
            kernel,
            name="mlp_qkv",
            out_shape=[
                jax.ShapeDtypeStruct((2, CHUNKS, NY, 2, piece, width), BF16),
                jax.ShapeDtypeStruct((qn, tokens), BF16),
                jax.ShapeDtypeStruct((n_ent * ff, width), BF16),
                jax.ShapeDtypeStruct((2 * NY * qn, hidden), BF16),
            ],
            in_specs=[ANY] * 7,
            out_specs=[ANY] * 4,
            scratch_shapes=[
                pltpu.VMEM((n_ent, half, width), BF16),
                pltpu.VMEM((2, hidden, ff), BF16),
                pltpu.VMEM((2, hidden, ff), BF16),
                pltpu.VMEM((half, n_ent * ff), BF16),
                pltpu.VMEM((SLOTS, 2, NY, piece, width), F32),
                pltpu.VMEM((TILES, 2, piece, width), F32),
                pltpu.VMEM((TILES, 4, piece, width), F32),
                pltpu.VMEM((2, TILES, piece, width), BF16),
                pltpu.VMEM((2 * piece, hidden), BF16),
                pltpu.VMEM((n_ent, 1, width), F32),
                pltpu.VMEM((n_ent, 1, width), F32),
                pltpu.VMEM((CHUNKS, 2 * NY, qn, 2 * piece), BF16),
                DMA((n_in,)),
                DMA((n_in,)),
                DMA((14, TILES)),
                DMA((14, TILES)),
                DMA((11,)),
                DMA((11,)),
                DMA((7, TILES)),
                DMA((7, TILES)),
                DMA((CHUNKS, 2 * NY)),
                DMA((CHUNKS, 2 * NY)),
                DMA((NY * SY + 2 * SX + 4,)),
                DMA((TILES,)),
                DMA((CHUNKS,)),
                pltpu.SemaphoreType.REGULAR,
            ],
            compiler_params=pltpu.CompilerParams(collective_id=1, has_side_effects=True, vmem_limit_bytes=LIMIT),
        )(residual, gain_mlp[None], gain_attn[None], w_gate, w_up, w_down, w_qkv.T)
        parts = 2
        resid, qkv_t = pl.pallas_call(
            hand_over,
            name="hand_over",
            out_shape=[jax.ShapeDtypeStruct((tokens, width), BF16), jax.ShapeDtypeStruct((qn, tokens), BF16)],
            in_specs=[ANY] * 2,
            out_specs=[ANY] * 2,
            scratch_shapes=[
                pltpu.VMEM((tokens, width), BF16),
                pltpu.VMEM((qn, tokens), BF16),
                DMA((parts,)),
                DMA((parts,)),
                DMA((2,)),
            ],
        )(resid.reshape(tokens, width), qkv_t)
        return resid, qkv_t.T

    return jax.shard_map(
        per_device,
        mesh=mesh,
        in_specs=(tok_spec, gain_spec, gain_spec, wide_spec, wide_spec, down_spec, wide_spec),
        out_specs=(tok_spec, qkv_spec),
        check_vma=False,
    )
```
